128 devices in a mesh: seq: 32 (over y, x, core), tp: 4 (over z).
Axes of the slice: x: 4, y: 4, z: 4, core: 2. Of those that a mesh axis runs over, the one named last changes fastest.
Arguments:
- hidden: bfloat16 [32768, 2560], P('seq', 'tp'), may hold values from -6 to 6
- gate_proj: bfloat16 [2560, 5120], P(None, 'tp'), may hold values from -0.125 to 0.125
- input_proj: bfloat16 [2560, 5120], P(None, 'tp'), may hold values from -0.125 to 0.125
- bc_proj: bfloat16 [2560, 256], replicated, may hold values from -0.125 to 0.125
- step_proj: bfloat16 [2560, 80], P(None, 'tp'), may hold values from -0.125 to 0.125
- step_bias: float32 [80], P('tp'), may hold values from -16 to -3
- decay_log: float32 [80], P('tp'), may hold values from 0 to 2.78
- conv_weight: float32 [4, 5120], P(None, 'tp'), may hold values from -3 to 3
- conv_bias: float32 [5120], P('tp'), may hold values from -3 to 3
- bc_conv_weight: float32 [4, 256], replicated, may hold values from -3 to 3
- bc_conv_bias: float32 [256], replicated, may hold values from -3 to 3
- skip_gain: float32 [80], P('tp'), may hold values from 0.5 to 2
- norm_gain: float32 [5120], P('tp'), may hold values from 0.1 to 1.9
- out_proj: bfloat16 [5120, 2560], P('tp'), may hold values from -0.078125 to 0.078125
- amax_history: float32 [16], replicated, may hold values from 1.5 to 4
Outputs:
- mixed: bfloat16 [32768, 2560], P('seq', 'tp')
- new_history: float32 [16], replicated
The draws below stay inside these ranges and needn't reach their ends.
All inputs are finite; a program needn't handle non-finite values.
Results may differ from the reference program's by a relative error of at most 0.015.
Values may be sent and summed in bfloat16 or wider, within the bound.
A program may use at most 192 MiB of HBM per device.

```python
import math
import jax
import jax.numpy as jnp
from jax import lax

D = 2560
HEADS = 80
HEAD_DIM = 64
STATE = 128
CONV = 4
BLOCK = 256
HIST = 16
INNER = 5120
TOKENS = 32768


def head_rates(key):
    base_key = jax.random.fold_in(key, 7)
    key_rate, key_kind, key_slow, key_fast = jax.random.split(base_key, 4)
    decay_rate = jnp.exp(jax.random.uniform(key_rate, (HEADS,), jnp.float32, 0.0, math.log(16.0)))
    slow_share = 0.5
    slow_heads = jax.random.uniform(key_kind, (HEADS,), jnp.float32) < slow_share
    slow_rate = jax.random.uniform(key_slow, (HEADS,), jnp.float32, 0.3, 1.5) / TOKENS
    fast_rate = 1.0 / jax.random.uniform(key_fast, (HEADS,), jnp.float32, 30.0, 50.0)
    mean_rate = jnp.where(slow_heads, slow_rate, fast_rate)
    return (decay_rate, mean_rate / decay_rate)


def draw_decay_log(key, part):
    decay_rate, step_mean = head_rates(key)
    return jnp.log(decay_rate).astype(jnp.float32)


def draw_step_bias(key, part):
    decay_rate, step_mean = head_rates(key)
    return jnp.log(jnp.expm1(step_mean)).astype(jnp.float32)


def levels(key, extent, shards, least, largest):
    factor_of = 1.0
    for dim, blocks in shards:
        heights = jax.random.uniform(jax.random.fold_in(jax.random.fold_in(key, 6), dim), (blocks,), jnp.float32, least / len(shards), largest / len(shards))
        factor_of = factor_of * jnp.repeat(jnp.exp(heights), extent[dim] // blocks).reshape((-1,) + (1,) * (len(extent) - 1 - dim))
    return factor_of


def bell_draw(own_key, extent, width, most, cuts=(), kind=jnp.bfloat16):
    values = width * jax.random.normal(own_key, extent, jnp.float32)
    if cuts:
        values = values * levels(own_key, extent, cuts, -0.22, 0.18)
    return jnp.clip(values, -most, most).astype(kind)


def setup_inputs(seed: int = 0) -> dict:
    key_of = jax.random.split(jax.random.key(seed), 16)
    hidden = bell_draw(key_of[0], (TOKENS, D), 1.0, 6.0, ((0, 32), (1, 4)))
    gate_proj = bell_draw(key_of[1], (D, INNER), D ** -0.5, 0.125, ((1, 4),))
    input_proj = bell_draw(key_of[2], (D, INNER), D ** -0.5, 0.125, ((1, 4),))
    bc_proj = bell_draw(key_of[3], (D, 2 * STATE), D ** -0.5, 0.125)
    step_proj = bell_draw(key_of[4], (D, HEADS), D ** -0.5, 0.125, ((1, 4),))
    step_bias = draw_step_bias(jax.random.fold_in(key_of[15], 71), 0)
    decay_log = draw_decay_log(jax.random.fold_in(key_of[15], 71), 0)
    conv_weight = bell_draw(key_of[7], (CONV, INNER), CONV ** -0.5, 3.0, ((1, 4),), jnp.float32)
    conv_bias = bell_draw(key_of[8], (INNER,), 0.5, 3.0, ((0, 4),), jnp.float32)
    bc_conv_weight = bell_draw(key_of[9], (CONV, 2 * STATE), CONV ** -0.5, 3.0, (), jnp.float32)
    bc_conv_bias = bell_draw(key_of[10], (2 * STATE,), 0.5, 3.0, (), jnp.float32)
    skip_gain = jnp.clip(0.5 + 1.5 * jax.random.uniform(key_of[11], (HEADS,), jnp.float32) ** levels(key_of[11], (HEADS,), ((0, 4),), -0.2, 0.2), 0.5, 2.0)
    norm_gain = jnp.clip(1.0 + 0.18 * jax.random.normal(key_of[12], (INNER,), jnp.float32), 0.1, 1.9)
    out_proj = bell_draw(key_of[13], (INNER, D), INNER ** -0.5, 0.078125, ((0, 4),))
    amax_history = jnp.clip(jax.random.uniform(key_of[14], (HIST,), jnp.float32, 1.5, 4.0), 1.5, 4.0)
    return {"hidden": hidden, "gate_proj": gate_proj, "input_proj": input_proj, "bc_proj": bc_proj, "step_proj": step_proj, "step_bias": step_bias, "decay_log": decay_log, "conv_weight": conv_weight, "conv_bias": conv_bias, "bc_conv_weight": bc_conv_weight, "bc_conv_bias": bc_conv_bias, "skip_gain": skip_gain, "norm_gain": norm_gain, "out_proj": out_proj, "amax_history": amax_history}


QMAX = 448.0
EPS = 1e-05

def conv_silu(pre_conv, weight, conv_shift):
    row_count = pre_conv.shape[0]
    kernel = weight.shape[0]
    padded = jnp.concatenate([jnp.zeros((kernel - 1, pre_conv.shape[1]), jnp.bfloat16), pre_conv], axis=0)
    running = jnp.zeros(pre_conv.shape, jnp.float32)
    for offset in range(kernel):
        running = running + weight[offset] * padded[offset:offset + row_count].astype(jnp.float32)
    return jax.nn.silu(running + conv_shift).astype(jnp.bfloat16)

def ssd_block(carry_state, block_data):
    x_block, b_block, c_block, step_block, decay_block = block_data
    length = x_block.shape[0]
    head_count = carry_state.shape[0]
    head_width = carry_state.shape[1]
    cum_decay = jnp.cumsum(decay_block, axis=1)
    scores = jnp.dot(c_block, b_block.T, preferred_element_type=jnp.float32)
    causal = lax.broadcasted_iota(jnp.int32, (length, length), 0) >= lax.broadcasted_iota(jnp.int32, (length, length), 1)
    decay_gap = cum_decay[:, :, None] - cum_decay[:, None, :]
    decay_mask = jnp.where(causal, jnp.exp(jnp.where(causal, decay_gap, 0.0)), 0.0)
    weights = (scores[None] * decay_mask * step_block[:, None, :]).astype(jnp.bfloat16)
    x_heads = x_block.reshape(length, head_count, head_width)
    intra_out = jnp.einsum('hts,shp->htp', weights.astype(jnp.float32), x_heads.astype(jnp.float32))
    inter_out = jnp.exp(cum_decay)[:, :, None] * jnp.einsum('tn,hpn->htp', c_block.astype(jnp.float32), carry_state, precision=lax.Precision.HIGHEST)
    tail_decay = jnp.exp(cum_decay[:, -1:] - cum_decay) * step_block
    x_weighted = (tail_decay.T[:, :, None] * x_heads.astype(jnp.float32)).astype(jnp.bfloat16)
    update = jnp.einsum('shp,sn->hpn', x_weighted.astype(jnp.float32), b_block.astype(jnp.float32))
    next_state = jnp.exp(cum_decay[:, -1])[:, None, None] * carry_state + update
    block_out = (intra_out + inter_out).transpose(1, 0, 2).reshape(length, head_count * head_width)
    return (next_state, block_out)

def reference(hidden, gate_proj, input_proj, bc_proj, step_proj, step_bias, decay_log, conv_weight, conv_bias, bc_conv_weight, bc_conv_bias, skip_gain, norm_gain, out_proj, amax_history):
    gate_in = jnp.dot(hidden, gate_proj, preferred_element_type=jnp.float32).astype(jnp.bfloat16)
    x_pre = jnp.dot(hidden, input_proj, preferred_element_type=jnp.float32).astype(jnp.bfloat16)
    bc_pre = jnp.dot(hidden, bc_proj, preferred_element_type=jnp.float32).astype(jnp.bfloat16)
    step_raw = jnp.dot(hidden, step_proj, preferred_element_type=jnp.float32)
    x_conv = conv_silu(x_pre, conv_weight, conv_bias)
    bc_conv = conv_silu(bc_pre, bc_conv_weight, bc_conv_bias)
    b_in = bc_conv[:, :STATE]
    c_out = bc_conv[:, STATE:]
    step_size = jax.nn.softplus(step_raw + step_bias)
    log_decay = step_size * -jnp.exp(decay_log)
    blocks = TOKENS // BLOCK
    stacked = (x_conv.reshape(blocks, BLOCK, INNER), b_in.reshape(blocks, BLOCK, STATE), c_out.reshape(blocks, BLOCK, STATE), step_size.reshape(blocks, BLOCK, HEADS).transpose(0, 2, 1), log_decay.reshape(blocks, BLOCK, HEADS).transpose(0, 2, 1))
    start_state = jnp.zeros((HEADS, HEAD_DIM, STATE), jnp.float32)
    final_state, block_outs = lax.scan(ssd_block, start_state, stacked)
    ssm_out = block_outs.reshape(TOKENS, INNER)
    x_heads = x_conv.reshape(TOKENS, HEADS, HEAD_DIM).astype(jnp.float32)
    ssm_out = ssm_out + (skip_gain[:, None] * x_heads).reshape(TOKENS, INNER)
    gated = ssm_out * jax.nn.silu(gate_in.astype(jnp.float32))
    inv_rms = lax.rsqrt(lax.optimization_barrier(jnp.mean(gated * gated, axis=1)) + EPS)
    normed = gated * inv_rms[:, None] * norm_gain
    peak_value = jnp.max(jnp.abs(normed))
    scale = QMAX / jnp.max(amax_history)
    quant = jnp.clip(normed * scale, -QMAX, QMAX).astype(jnp.bfloat16)
    mixed = (jnp.dot(quant, out_proj, preferred_element_type=jnp.float32) / scale).astype(jnp.bfloat16)
    new_history = jnp.concatenate([peak_value.reshape(1), amax_history[:-1]])
    return (mixed, new_history)
```

```python
import types

import jax
import jax.numpy as jnp
from jax import lax
from jax.experimental import pallas as pl
from jax.experimental.pallas import tpu as pltpu
from jax.sharding import PartitionSpec as P

QMAX = 448.0
EPS = 1e-05
HEAD = 64
LANES = 128
CHUNK = 128
RIM = 8
TAIL = 16
MESH = pl.DeviceIdType.MESH
F32 = jnp.float32
BF16 = jnp.bfloat16


def dot(a, b):
    return jnp.dot(a, b, preferred_element_type=F32)


def half_silu(v):
    half = 0.5 * v
    return half + half * jnp.tanh(half)


def softplus(v):
    u = jnp.exp(-jnp.abs(v))
    s = u / (2.0 + u)
    q = s * s
    series = jnp.full_like(q, 1.0 / 15.0)
    for k in (13, 11, 9, 7, 5, 3, 1):
        series = series * q + 1.0 / k
    return jnp.maximum(v, 0.0) + 2.0 * s * series


def conv_silu(window, weight, shift):
    total = shift + weight[3:4] * window[RIM:]
    for k in range(3):
        total = total + weight[k : k + 1] * pltpu.roll(window, 3 - k, 0)[RIM:]
    return half_silu(total)


def running_sum(lower, v):
    top = v.astype(BF16)
    rest = v - top.astype(F32)
    middle = rest.astype(BF16)
    last = (rest - middle.astype(F32)).astype(BF16)
    return dot(lower, top) + (dot(lower, middle) + dot(lower, last))


def pair_of(v, k, rows):
    low = lax.broadcasted_iota(jnp.int32, (rows, LANES), 1) < HEAD
    first = jnp.broadcast_to(v[:, 2 * k : 2 * k + 1], (rows, LANES))
    second = jnp.broadcast_to(v[:, 2 * k + 1 : 2 * k + 2], (rows, LANES))
    return first, second, jnp.where(low, first, second)


def build(rows, part, inner, n_tp, n_seq, heads):
    depth = part * n_tp
    pairs = heads // 2
    block = min(256, rows // 2)
    blocks = rows // block
    half = block // 2
    chunks = rows // CHUNK
    per = block // CHUNK
    slice_rows = max(8, LANES // n_seq)
    lane_parts = n_seq * slice_rows // LANES
    slice_lanes = inner // lane_parts
    ntile = 256

    vmem = {
        "h": ((rows, depth), BF16),
        "tail": ((TAIL, depth), BF16),
        "wg": ((depth, inner), BF16),
        "wx": ((depth, inner), BF16),
        "wb": ((depth, 2 * LANES), BF16),
        "ws": ((depth, LANES), BF16),
        "wo": ((inner, depth), BF16),
        "xp": ((rows + RIM, inner), F32),
        "bp": ((rows + RIM, 2 * LANES), F32),
        "sp": ((rows, LANES), F32),
        "gs": ((rows, inner), BF16),
        "ys": ((rows, inner), F32),
        "cs": ((rows, LANES), BF16),
        "cd": ((rows, LANES), F32),
        "yi": ((CHUNK, inner), F32),
        "xw": ((CHUNK, inner), BF16),
        "state": ((LANES, inner), F32),
        "dexp": ((1, inner), F32),
        "run": ((1, LANES), F32),
        "bias": ((1, LANES), F32),
        "rate": ((1, LANES), F32),
        "rimx": ((TAIL, inner), F32),
        "rimb": ((TAIL, 2 * LANES), F32),
        "stx": ((n_seq, slice_rows, slice_lanes), BF16),
        "srx": ((n_seq, slice_rows, slice_lanes), BF16),
        "ptx": ((n_seq, slice_rows, slice_lanes), BF16),
        "prx": ((n_seq, slice_rows, slice_lanes), BF16),
        "dtx": ((lane_parts, 1, slice_lanes), F32),
        "drx": ((n_seq, 1, slice_lanes), F32),
        "sin": ((LANES, inner), F32),
        "stat": ((n_tp, chunks, 8, LANES), F32),
        "tr": ((rows, part), BF16),
        "rl": ((rows // 2, part), BF16),
        "rr": ((rows // 2, part), BF16),
        "txp": ((rows, part), BF16),
        "txm": ((rows, part), BF16),
        "rxp": ((rows, part), BF16),
        "rxm": ((rows, part), BF16),
        "peak": ((1, LANES), F32),
        "pkt": ((1, LANES), F32),
        "pkr": ((n_seq, 1, LANES), F32),
    }
    dma = {
        "load": 7,
        "own_ps": blocks, "own_ms": blocks, "own_pr": blocks, "own_mr": blocks,
        "rel_ps": blocks, "rel_ms": blocks, "rel_pr": blocks, "rel_mr": blocks,
        "tail_s": n_tp, "tail_r": n_tp,
        "rim_s": 2, "rim_r": 2,
        "st_s": n_seq, "st_r": n_seq, "dc_s": n_seq, "dc_r": n_seq,
        "pf_s": n_seq, "pf_r": n_seq, "pk_s": n_seq, "pk_r": n_seq,
        "sa_s": chunks * n_tp, "sa_r": chunks * n_tp,
        "far_ps": blocks, "far_ms": blocks, "far_pr": blocks, "far_mr": blocks,
        "near_ps": blocks, "near_ms": blocks, "near_pr": blocks, "near_mr": blocks,
    }
    inputs = (
        "hidden", "gate_w", "in_w", "bc_w", "step_w", "step_b", "dlog", "conv_w", "conv_b",
        "bcc_w", "bcc_b", "skip", "gain", "out_w", "hist",
    )
    outputs = ("mixed", "news")
    names = (*inputs, *outputs, *vmem, *dma)

    def kernel(*refs):
        r = types.SimpleNamespace(**dict(zip(names, refs)))
        me = lax.axis_index("tp")
        at = lax.axis_index("seq")
        right = lax.rem(me + 1, n_tp)
        left = lax.rem(me + n_tp - 1, n_tp)
        opp = lax.rem(me + 2, n_tp)

        def cols(q):
            return pl.ds(pl.multiple_of(q * part, LANES), part)

        def brows(b):
            return pl.ds(pl.multiple_of(b * block, block), block)

        def hrows(b, side):
            return pl.ds(pl.multiple_of(b * block + side * half, half), half)

        def halfrows(b):
            return pl.ds(pl.multiple_of(b * half, half), half)

        def crows(k):
            return pl.ds(pl.multiple_of(k * CHUNK, CHUNK), CHUNK)

        def to_tp(src, dst, send, recv, q):
            return pltpu.make_async_remote_copy(
                src_ref=src, dst_ref=dst, send_sem=send, recv_sem=recv,
                device_id={"tp": q}, device_id_type=MESH,
            )

        def to_seq(src, dst, send, recv, q):
            return pltpu.make_async_remote_copy(
                src_ref=src, dst_ref=dst, send_sem=send, recv_sem=recv,
                device_id={"seq": q}, device_id_type=MESH,
            )

        loads = [
            pltpu.make_async_copy(src, dst, r.load.at[i])
            for i, (src, dst) in enumerate((
                (r.hidden, r.h.at[:, cols(me)]),
                (r.hidden.at[pl.ds(rows - TAIL, TAIL), :], r.tail.at[:, cols(me)]),
                (r.in_w, r.wx), (r.bc_w, r.wb), (r.gate_w, r.wg), (r.out_w, r.wo),
            ))
        ]
        for c in loads:
            c.start()

        barrier = pltpu.get_barrier_semaphore()
        for off in range(1, n_tp):
            pl.semaphore_signal(
                barrier, inc=1, device_id={"tp": lax.rem(me + off, n_tp)}, device_id_type=MESH
            )

        def greet(off, _):
            pl.semaphore_signal(
                barrier, inc=1, device_id={"seq": lax.rem(at + off, n_seq)}, device_id_type=MESH
            )
            return 0

        lax.fori_loop(1, n_seq, greet, 0)
        pl.semaphore_wait(barrier, n_tp - 1 + n_seq - 1)

        def own_p(b):
            here = r.h.at[brows(b), cols(me)]
            return to_tp(here, here, r.own_ps.at[b], r.own_pr.at[b], right)

        def own_m(b):
            here = r.h.at[brows(b), cols(me)]
            return to_tp(here, here, r.own_ms.at[b], r.own_mr.at[b], left)

        def rel_p(b):
            here = r.h.at[hrows(b, 0), cols(left)]
            return to_tp(here, here, r.rel_ps.at[b], r.rel_pr.at[b], right)

        def rel_m(b):
            here = r.h.at[hrows(b, 1), cols(right)]
            return to_tp(here, here, r.rel_ms.at[b], r.rel_mr.at[b], left)

        def got(view, sem):
            pltpu.make_async_copy(view, view, sem).wait()

        loads[1].wait()
        tails = []
        for off in range(1, n_tp):
            here = r.tail.at[:, cols(me)]
            tails.append(to_tp(
                here, here, r.tail_s.at[off], r.tail_r.at[off], lax.rem(me + off, n_tp)
            ))
            tails[-1].start()
        loads[0].wait()
        for b in range(2):
            own_p(b).start()
            own_m(b).start()

        r.ws[...] = jnp.zeros_like(r.ws)
        r.ws[:, :heads] = r.step_w[...]
        r.bias[...] = jnp.zeros_like(r.bias)
        r.bias[:, :heads] = r.step_b[...]
        r.rate[...] = jnp.zeros_like(r.rate)
        r.rate[:, :heads] = -jnp.exp(r.dlog[...])
        r.run[...] = jnp.zeros_like(r.run)
        r.state[...] = jnp.zeros_like(r.state)

        loads[2].wait()
        loads[3].wait()
        for off in range(1, n_tp):
            src = lax.rem(me + n_tp - off, n_tp)
            got(r.tail.at[:, cols(src)], r.tail_r.at[off])

        def rim_tile(n, _):
            lanes = pl.ds(pl.multiple_of(n * ntile, ntile), ntile)
            r.rimx[:, lanes] = dot(r.tail[...], r.wx[:, lanes])
            return 0

        lax.fori_loop(0, inner // ntile, rim_tile, 0)
        r.rimb[...] = dot(r.tail[...], r.wb[...])
        ahead = lax.rem(at + 1, n_seq)
        rims = (
            to_seq(r.rimx.at[pl.ds(TAIL - RIM, RIM), :], r.xp.at[pl.ds(0, RIM), :],
                   r.rim_s.at[0], r.rim_r.at[0], ahead),
            to_seq(r.rimb.at[pl.ds(TAIL - RIM, RIM), :], r.bp.at[pl.ds(0, RIM), :],
                   r.rim_s.at[1], r.rim_r.at[1], ahead),
        )

        @pl.when(at < n_seq - 1)
        def _():
            for c in rims:
                c.start()

        @pl.when(at == 0)
        def _():
            r.xp[0:RIM, :] = jnp.zeros((RIM, inner), F32)
            r.bp[0:RIM, :] = jnp.zeros((RIM, 2 * LANES), F32)

        def project(b):
            mine = brows(b)
            after = pl.ds(pl.multiple_of(b * block + RIM, 8), block)
            r.bp[after, :] = dot(r.h[mine, :], r.wb[...])
            r.sp[mine, :] = dot(r.h[mine, :], r.ws[...])

            def tile(n, _):
                lanes = pl.ds(pl.multiple_of(n * ntile, ntile), ntile)
                r.xp[after, lanes] = dot(r.h[mine, :], r.wx[:, lanes])
                return 0

            lax.fori_loop(0, inner // ntile, tile, 0)

        def project_gate(b):
            mine = brows(b)

            def tile(n, _):
                lanes = pl.ds(pl.multiple_of(n * ntile, ntile), ntile)
                r.gs[mine, lanes] = dot(r.h[mine, :], r.wg[:, lanes]).astype(BF16)
                return 0

            lax.fori_loop(0, inner // ntile, tile, 0)

        def recur(k):
            mine = crows(k)
            window = pl.ds(pl.multiple_of(k * CHUNK, CHUNK), CHUNK + RIM)
            bc = conv_silu(r.bp[window, :], r.bcc_w[...], r.bcc_b[...])
            b_t = bc[:, :LANES].T.astype(BF16)
            c_in = bc[:, LANES:].astype(BF16)
            r.cs[mine, :] = c_in
            down = lax.broadcasted_iota(jnp.int32, (CHUNK, CHUNK), 0)
            across = lax.broadcasted_iota(jnp.int32, (CHUNK, CHUNK), 1)
            causal = down >= across
            scores = jnp.where(causal, dot(c_in, b_t), 0.0)
            step = softplus(r.sp[mine, :] + r.bias[...])
            cum = running_sum(jnp.where(causal, 1.0, 0.0).astype(BF16), step * r.rate[...])
            cum_t = cum.T
            end = cum[CHUNK - 1 :, :]
            r.cd[mine, :] = cum + r.run[...]
            r.run[...] = r.run[...] + end
            r.yi[...] = dot(c_in, r.state[...].astype(BF16))
            low = lax.broadcasted_iota(jnp.int32, (CHUNK, LANES), 1) < HEAD
            for k2 in range(pairs):
                lanes = slice(k2 * LANES, (k2 + 1) * LANES)
                x = conv_silu(r.xp[window, lanes], r.conv_w[:, lanes], r.conv_b[:, lanes])
                first, second, both = pair_of(cum, k2, CHUNK)
                _, _, steps = pair_of(step, k2, CHUNK)
                last = both[CHUNK - 1 :, :]
                x_step = x * steps
                r.xw[:, lanes] = (jnp.exp(last - both) * x_step).astype(BF16)
                r.dexp[:, lanes] = jnp.exp(last)
                rise = [
                    (scores * jnp.exp(jnp.minimum(v - cum_t[2 * k2 + i : 2 * k2 + i + 1, :], 0.0)))
                    .astype(BF16)
                    for i, v in enumerate((first, second))
                ]
                fed = jnp.concatenate(
                    [jnp.where(low, x_step, 0.0), jnp.where(low, 0.0, x_step)], axis=0
                ).astype(BF16)
                _, _, kept = pair_of(r.skip[...], k2, 1)
                y = dot(jnp.concatenate(rise, axis=1), fed)
                r.ys[mine, lanes] = y + jnp.exp(both) * r.yi[:, lanes] + kept * x
            r.state[...] = r.dexp[...] * r.state[...] + dot(b_t, r.xw[...])

        def gather_step(b, _):
            @pl.when(b < blocks)
            def _():
                got(r.h.at[brows(b), cols(left)], r.own_pr.at[b])
                rel_p(b).start()
                got(r.h.at[brows(b), cols(right)], r.own_mr.at[b])
                rel_m(b).start()

                @pl.when(b + 2 < blocks)
                def _():
                    own_p(b + 2).start()
                    own_m(b + 2).start()

            @pl.when(b == 1)
            def _():
                @pl.when(at > 0)
                def _():
                    got(r.xp.at[pl.ds(0, RIM), :], r.rim_r.at[0])
                    got(r.bp.at[pl.ds(0, RIM), :], r.rim_r.at[1])

            @pl.when(b > 0)
            def _():
                done = b - 1
                got(r.h.at[hrows(done, 0), cols(opp)], r.rel_pr.at[done])
                got(r.h.at[hrows(done, 1), cols(opp)], r.rel_mr.at[done])
                project(done)
                lax.fori_loop(0, per, lambda j, _: (recur(done * per + j), 0)[1], 0)

            return 0

        lax.fori_loop(0, blocks + 1, gather_step, 0)

        for j in range(n_seq):
            top = (j // lane_parts) * slice_rows
            lane = (j % lane_parts) * slice_lanes
            r.stx[j] = r.state[top : top + slice_rows, lane : lane + slice_lanes].astype(BF16)
        for k2 in range(pairs):
            lanes = slice(k2 * LANES, (k2 + 1) * LANES)
            _, _, both = pair_of(r.run[...], k2, 1)
            r.dexp[:, lanes] = jnp.exp(both)
        for j in range(lane_parts):
            r.dtx[j] = r.dexp[:, j * slice_lanes : (j + 1) * slice_lanes]

        def state_to(off):
            q = lax.rem(at + off, n_seq)
            return (
                to_seq(r.stx.at[q], r.srx.at[at], r.st_s.at[off], r.st_r.at[off], q),
                to_seq(r.dtx.at[lax.rem(q, lane_parts)], r.drx.at[at],
                       r.dc_s.at[off], r.dc_r.at[off], q),
            )

        def state_send(off, _):
            for c in state_to(off):
                c.start()
            return 0

        lax.fori_loop(1, n_seq, state_send, 0)
        r.srx[at] = r.stx[at]
        r.drx[at] = r.dtx[lax.rem(at, lane_parts)]
        loads[4].wait()
        early = blocks // 2
        lax.fori_loop(0, early, lambda b, _: (project_gate(b), 0)[1], 0)

        def state_got(off, _):
            q = lax.rem(at + n_seq - off, n_seq)
            got(r.srx.at[q], r.st_r.at[off])
            got(r.drx.at[q], r.dc_r.at[off])
            return 0

        lax.fori_loop(1, n_seq, state_got, 0)

        def scan(j, before):
            r.ptx[j] = before.astype(BF16)
            return r.drx[j] * before + r.srx[j].astype(F32)

        lax.fori_loop(0, n_seq, scan, jnp.zeros((slice_rows, slice_lanes), F32))

        def prefix_to(off):
            q = lax.rem(at + off, n_seq)
            return to_seq(r.ptx.at[q], r.prx.at[at], r.pf_s.at[off], r.pf_r.at[off], q)

        def prefix_send(off, _):
            prefix_to(off).start()
            return 0

        lax.fori_loop(1, n_seq, prefix_send, 0)
        r.prx[at] = r.ptx[at]
        lax.fori_loop(early, blocks, lambda b, _: (project_gate(b), 0)[1], 0)

        def prefix_got(off, _):
            got(r.prx.at[lax.rem(at + n_seq - off, n_seq)], r.pf_r.at[off])
            return 0

        lax.fori_loop(1, n_seq, prefix_got, 0)
        for j in range(n_seq):
            top = (j // lane_parts) * slice_rows
            lane = (j % lane_parts) * slice_lanes
            r.sin[top : top + slice_rows, lane : lane + slice_lanes] = r.prx[j].astype(F32)

        def stat_to(k, off):
            here = r.stat.at[me, k]
            i = k * n_tp + off
            return to_tp(here, here, r.sa_s.at[i], r.sa_r.at[i], lax.rem(me + off, n_tp))

        def gate(k, _):
            mine = crows(k)
            r.yi[...] = dot(r.cs[mine, :], r.sin[...].astype(BF16))
            reach = r.cd[mine, :]
            squares = jnp.zeros((CHUNK, LANES), F32)
            tops = jnp.zeros((CHUNK, LANES), F32)
            for k2 in range(pairs):
                lanes = slice(k2 * LANES, (k2 + 1) * LANES)
                _, _, both = pair_of(reach, k2, CHUNK)
                out = r.ys[mine, lanes] + jnp.exp(both) * r.yi[:, lanes]
                gated = out * half_silu(r.gs[mine, lanes].astype(F32))
                squares = squares + gated * gated
                gained = gated * r.gain[:, lanes]
                tops = jnp.maximum(tops, jnp.abs(gained))
                r.ys[mine, lanes] = gained
            r.stat[me, k, 0:1, :] = jnp.sum(squares.T, axis=0, keepdims=True)
            r.stat[me, k, 1:2, :] = jnp.max(tops.T, axis=0, keepdims=True)
            for off in range(1, n_tp):
                stat_to(k, off).start()
            return 0

        lax.fori_loop(0, chunks, gate, 0)

        most = r.hist[0]
        for i in range(1, r.hist.shape[0]):
            most = jnp.maximum(most, r.hist[i])
        unscale = jnp.full((1, LANES), most, F32) / QMAX
        scale = QMAX / jnp.full((1, LANES), most, F32)
        r.peak[...] = jnp.zeros_like(r.peak)
        loads[5].wait()

        def norm(k):
            mine = crows(k)
            for off in range(1, n_tp):
                got(r.stat.at[lax.rem(me + n_tp - off, n_tp), k], r.sa_r.at[k * n_tp + off])
            squares = r.stat[0, k, 0:1, :]
            tops = r.stat[0, k, 1:2, :]
            for q in range(1, n_tp):
                squares = squares + r.stat[q, k, 0:1, :]
                tops = jnp.maximum(tops, r.stat[q, k, 1:2, :])
            inv = lax.rsqrt(squares * (1.0 / (inner * n_tp)) + EPS)
            r.peak[...] = jnp.maximum(r.peak[...], tops * inv)
            factor = jnp.broadcast_to(inv * scale, (CHUNK, LANES)).T
            for k2 in range(pairs):
                lanes = slice(k2 * LANES, (k2 + 1) * LANES)
                r.gs[mine, lanes] = jnp.clip(r.ys[mine, lanes] * factor, -QMAX, QMAX).astype(BF16)

        def far_p(b):
            return to_tp(r.tr.at[hrows(b, 0), :], r.rl.at[halfrows(b), :],
                         r.far_ps.at[b], r.far_pr.at[b], right)

        def far_m(b):
            return to_tp(r.tr.at[hrows(b, 1), :], r.rr.at[halfrows(b), :],
                         r.far_ms.at[b], r.far_mr.at[b], left)

        def near_p(b):
            return to_tp(r.txp.at[brows(b), :], r.rxp.at[brows(b), :],
                         r.near_ps.at[b], r.near_pr.at[b], right)

        def near_m(b):
            return to_tp(r.txm.at[brows(b), :], r.rxm.at[brows(b), :],
                         r.near_ms.at[b], r.near_mr.at[b], left)

        def far(b, _):
            lax.fori_loop(0, per, lambda j, _: (norm(b * per + j), 0)[1], 0)
            r.tr[brows(b), :] = dot(r.gs[brows(b), :], r.wo[:, cols(opp)]).astype(BF16)
            far_p(b).start()
            far_m(b).start()
            return 0

        lax.fori_loop(0, blocks, far, 0)
        r.pkt[...] = r.peak[...]

        def peak_to(off):
            q = lax.rem(at + off, n_seq)
            return to_seq(r.pkt, r.pkr.at[at], r.pk_s.at[off], r.pk_r.at[off], q)

        def peak_send(off, _):
            peak_to(off).start()
            return 0

        lax.fori_loop(1, n_seq, peak_send, 0)
        r.pkr[at] = r.peak[...]

        def near(b, _):
            mine = brows(b)
            r.txp[mine, :] = dot(r.gs[mine, :], r.wo[:, cols(right)]).astype(BF16)
            r.txm[mine, :] = dot(r.gs[mine, :], r.wo[:, cols(left)]).astype(BF16)
            got(r.rl.at[halfrows(b), :], r.far_pr.at[b])
            top = hrows(b, 0)
            r.txp[top, :] = (r.txp[top, :].astype(F32) + r.rl[halfrows(b), :].astype(F32)).astype(BF16)
            near_p(b).start()
            got(r.rr.at[halfrows(b), :], r.far_mr.at[b])
            low = hrows(b, 1)
            r.txm[low, :] = (r.txm[low, :].astype(F32) + r.rr[halfrows(b), :].astype(F32)).astype(BF16)
            near_m(b).start()
            return 0

        lax.fori_loop(0, blocks, near, 0)

        def finish(b, _):
            mine = brows(b)
            total = dot(r.gs[mine, :], r.wo[:, cols(me)])
            got(r.rxp.at[mine, :], r.near_pr.at[b])
            got(r.rxm.at[mine, :], r.near_mr.at[b])
            total = total + (r.rxp[mine, :].astype(F32) + r.rxm[mine, :].astype(F32))
            r.mixed[mine, :] = (total * unscale[0:1, 0:1]).astype(BF16)
            return 0

        lax.fori_loop(0, blocks, finish, 0)

        def peak_got(off, top):
            q = lax.rem(at + n_seq - off, n_seq)
            got(r.pkr.at[q], r.pk_r.at[off])
            return jnp.maximum(top, r.pkr[q])

        top = lax.fori_loop(1, n_seq, peak_got, r.pkr[at])
        r.news[0] = jnp.max(top)
        for i in range(1, r.hist.shape[0]):
            r.news[i] = r.hist[i - 1]

        for c in tails:
            c.wait_send()

        @pl.when(at < n_seq - 1)
        def _():
            for c in rims:
                c.wait_send()

        def sent_block(b, _):
            for make in (own_p, own_m, rel_p, rel_m, far_p, far_m, near_p, near_m):
                make(b).wait_send()
            return 0

        lax.fori_loop(0, blocks, sent_block, 0)

        def sent_seq(off, _):
            for c in (*state_to(off), prefix_to(off), peak_to(off)):
                c.wait_send()
            return 0

        lax.fori_loop(1, n_seq, sent_seq, 0)

        def sent_stat(k, _):
            for off in range(1, n_tp):
                stat_to(k, off).wait_send()
            return 0

        lax.fori_loop(0, chunks, sent_stat, 0)

    hbm = pl.BlockSpec(memory_space=pl.ANY)
    local = pl.BlockSpec(memory_space=pltpu.VMEM)
    scalars = pl.BlockSpec(memory_space=pltpu.SMEM)
    return pl.pallas_call(
        kernel,
        name="layer",
        out_shape=(
            jax.ShapeDtypeStruct((rows, part), BF16),
            jax.ShapeDtypeStruct((16,), F32),
        ),
        in_specs=[hbm] * 4 + [local] * 9 + [hbm, scalars],
        out_specs=(local, scalars),
        scratch_shapes=[pltpu.VMEM(*v) for v in vmem.values()]
        + [pltpu.SemaphoreType.DMA((n,)) for n in dma.values()],
        compiler_params=pltpu.CompilerParams(
            collective_id=0, has_side_effects=True, vmem_limit_bytes=67_043_328
        ),
    )


def solution(mesh):
    n_seq, n_tp = mesh.shape["seq"], mesh.shape["tp"]

    def shards(
        hidden, gate_proj, input_proj, bc_proj, step_proj, step_bias, decay_log, conv_weight,
        conv_bias, bc_conv_weight, bc_conv_bias, skip_gain, norm_gain, out_proj, amax_history,
    ):
        rows, part = hidden.shape
        call = build(rows, part, gate_proj.shape[1], n_tp, n_seq, step_proj.shape[1])
        return call(
            hidden, gate_proj, input_proj, bc_proj, step_proj, step_bias[None], decay_log[None],
            conv_weight, conv_bias[None], bc_conv_weight, bc_conv_bias[None], skip_gain[None],
            norm_gain[None], out_proj, amax_history,
        )

    cols = P(None, "tp")
    flat = P("tp")
    in_specs = (
        P("seq", "tp"), cols, cols, P(), cols, flat, flat, cols, flat, P(), P(), flat, flat,
        P("tp", None), P(),
    )
    return jax.shard_map(
        shards, mesh=mesh, in_specs=in_specs, out_specs=(P("seq", "tp"), P()), check_vma=False
    )
```

```python
import types

import jax
import jax.numpy as jnp
from jax import lax
from jax.experimental import pallas as pl
from jax.experimental.pallas import tpu as pltpu
from jax.sharding import PartitionSpec as P

QMAX = 448.0
EPS = 1e-05
HEAD = 64
LANES = 128
CHUNK = 128
RIM = 8
TAIL = 16
MESH = pl.DeviceIdType.MESH
F32 = jnp.float32
BF16 = jnp.bfloat16


def dot(a, b):
    return jnp.dot(a, b, preferred_element_type=F32)


def half_silu(v):
    half = 0.5 * v
    return half + half * jnp.tanh(half)


def softplus(v):
    u = jnp.exp(-jnp.abs(v))
    s = u / (2.0 + u)
    q = s * s
    series = jnp.full_like(q, 1.0 / 15.0)
    for k in (13, 11, 9, 7, 5, 3, 1):
        series = series * q + 1.0 / k
    return jnp.maximum(v, 0.0) + 2.0 * s * series


def conv_silu(window, weight, shift):
    total = shift + weight[3:4] * window[RIM:]
    for k in range(3):
        total = total + weight[k : k + 1] * pltpu.roll(window, 3 - k, 0)[RIM:]
    return half_silu(total)


def running_sum(lower, v):
    top = v.astype(BF16)
    rest = v - top.astype(F32)
    middle = rest.astype(BF16)
    last = (rest - middle.astype(F32)).astype(BF16)
    return dot(lower, top) + (dot(lower, middle) + dot(lower, last))


def pair_of(v, k, rows):
    low = lax.broadcasted_iota(jnp.int32, (rows, LANES), 1) < HEAD
    first = jnp.broadcast_to(v[:, 2 * k : 2 * k + 1], (rows, LANES))
    second = jnp.broadcast_to(v[:, 2 * k + 1 : 2 * k + 2], (rows, LANES))
    return first, second, jnp.where(low, first, second)


def build(rows, part, inner, n_tp, n_seq, heads, split):
    depth = part * n_tp
    pairs = heads // 2
    block = min(256, rows // 2)
    blocks = rows // block
    half = block // 2
    chunks = rows // CHUNK
    per = block // CHUNK
    piece = 128
    pieces = rows // piece
    most_depth = 3 * part
    slice_rows = max(8, LANES // n_seq)
    lane_parts = n_seq * slice_rows // LANES
    slice_lanes = inner // lane_parts
    ntile = 256

    vmem = {
        "h": ((rows, depth), BF16),
        "tail": ((TAIL, depth), BF16),
        "wg": ((depth, inner), BF16),
        "wx": ((depth, inner), BF16),
        "wb": ((depth, 2 * LANES), BF16),
        "ws": ((LANES, depth), BF16),
        "wo": ((inner, depth), BF16),
        "xp": ((rows + RIM, inner), F32),
        "bp": ((rows + RIM, 2 * LANES), F32),
        "sp": ((rows, LANES), F32),
        "gs": ((rows, inner), BF16),
        "ys": ((rows, inner), F32),
        "cs": ((rows, LANES), BF16),
        "cd": ((rows, LANES), F32),
        "yi": ((CHUNK, inner), F32),
        "xw": ((CHUNK, inner), BF16),
        "xc": ((CHUNK, inner), BF16),
        "fed": ((2 * CHUNK, inner), BF16),
        "bt": ((LANES, CHUNK), BF16),
        "cum": ((CHUNK, LANES), F32),
        "state": ((LANES, inner), F32),
        "dexp": ((1, inner), F32),
        "run": ((1, LANES), F32),
        "bias": ((1, LANES), F32),
        "rate": ((1, LANES), F32),
        "rimx": ((TAIL, inner), F32),
        "rimb": ((TAIL, 2 * LANES), F32),
        "stx": ((n_seq, slice_rows, slice_lanes), BF16),
        "srx": ((n_seq, slice_rows, slice_lanes), BF16),
        "ptx": ((n_seq, slice_rows, slice_lanes), BF16),
        "prx": ((n_seq, slice_rows, slice_lanes), BF16),
        "dtx": ((lane_parts, 1, slice_lanes), F32),
        "drx": ((n_seq, 1, slice_lanes), F32),
        "sin": ((LANES, inner), F32),
        "stat": ((n_tp, chunks, 8, LANES), F32),
        "tr": ((rows, part), BF16),
        "rl": ((rows // 2, part), BF16),
        "rr": ((rows // 2, part), BF16),
        "txp": ((rows, part), BF16),
        "txm": ((rows, part), BF16),
        "rxp": ((rows, part), BF16),
        "rxm": ((rows, part), BF16),
        "peak": ((1, LANES), F32),
        "pkt": ((1, LANES), F32),
        "pkr": ((n_seq, 1, LANES), F32),
    }
    dma = {
        "load": 6,
        "own_ps": 1, "own_ms": 1, "own_pr": pieces, "own_mr": pieces,
        "rel_ps": 1, "rel_ms": 1, "rel_pr": pieces, "rel_mr": pieces,
        "tail_s": 1, "tail_r": 1, "rim_s": 2, "rim_r": 2,
        "st_s": 1, "st_r": 1, "dc_s": 1, "dc_r": 1,
        "pf_s": 1, "pf_r": 1, "pk_s": 1, "pk_r": 1,
        "sa_s": 1, "sa_r": chunks,
        "far_ps": 1, "far_ms": 1, "far_pr": chunks, "far_mr": chunks,
        "near_ps": 1, "near_ms": 1, "near_pr": blocks, "near_mr": blocks,
    }
    inputs = (
        "hidden", "gate_w", "in_w", "bc_w", "step_w", "step_b", "dlog", "conv_w", "conv_b",
        "bcc_w", "bcc_b", "skip", "gain", "out_w", "hist",
    )
    outputs = ("mixed", "news")
    names = (*inputs, *outputs, *vmem, *dma)

    def kernel(*refs):
        r = types.SimpleNamespace(**dict(zip(names, refs)))
        me = lax.axis_index("tp")
        at = lax.axis_index("seq")
        right = lax.rem(me + 1, n_tp)
        left = lax.rem(me + n_tp - 1, n_tp)
        opp = lax.rem(me + 2, n_tp)

        def cols(q):
            return pl.ds(pl.multiple_of(q * part, LANES), part)

        def brows(b):
            return pl.ds(pl.multiple_of(b * block, block), block)

        def hrows(b, side):
            return pl.ds(pl.multiple_of(b * block + side * half, half), half)

        def halfrows(b):
            return pl.ds(pl.multiple_of(b * half, half), half)

        def crows(k):
            return pl.ds(pl.multiple_of(k * CHUNK, CHUNK), CHUNK)

        def to_tp(src, dst, send, recv, q):
            return pltpu.make_async_remote_copy(
                src_ref=src, dst_ref=dst, send_sem=send, recv_sem=recv,
                device_id={"tp": q}, device_id_type=MESH,
            )

        def to_seq(src, dst, send, recv, q):
            return pltpu.make_async_remote_copy(
                src_ref=src, dst_ref=dst, send_sem=send, recv_sem=recv,
                device_id={"seq": q}, device_id_type=MESH,
            )

        slot = [slice(i * part, (i + 1) * part) for i in range(n_tp)]
        before, own, after, far_side = slot
        known = slice(0, most_depth)
        order = (left, me, right, opp)

        def load(src, dst, i):
            return pltpu.make_async_copy(src, dst, r.load.at[i])

        first = [
            load(r.hidden, r.h.at[:, own], 0),
            load(r.hidden.at[pl.ds(rows - TAIL, TAIL), :], r.tail.at[:, own], 1),
        ]
        for c in first:
            c.start()

        def by_rows(src, dst, i):
            return [
                load(src.at[pl.ds(pl.multiple_of(q * part, LANES), part), :],
                     dst.at[pl.ds(j * part, part), :], i)
                for j, q in enumerate(order)
            ]

        weights = (
            by_rows(r.in_w, r.wx, 2) + by_rows(r.bc_w, r.wb, 3) + by_rows(r.gate_w, r.wg, 4)
            + [load(r.out_w, r.wo, 5)]
        )

        barrier = pltpu.get_barrier_semaphore()
        for off in range(1, n_tp):
            pl.semaphore_signal(
                barrier, inc=1, device_id={"tp": lax.rem(me + off, n_tp)}, device_id_type=MESH
            )

        def greet(off, _):
            pl.semaphore_signal(
                barrier, inc=1, device_id={"seq": lax.rem(at + off, n_seq)}, device_id_type=MESH
            )
            return 0

        lax.fori_loop(1, n_seq, greet, 0)
        pl.semaphore_wait(barrier, n_tp - 1 + n_seq - 1)

        def prows(b):
            return pl.ds(pl.multiple_of(b * piece, piece), piece)

        def phalf(b, side):
            return pl.ds(pl.multiple_of(b * piece + side * (piece // 2), piece // 2), piece // 2)

        def own_p(b):
            return to_tp(r.h.at[prows(b), own], r.h.at[prows(b), before],
                         r.own_ps.at[0], r.own_pr.at[b], right)

        def own_m(b):
            return to_tp(r.h.at[prows(b), own], r.h.at[prows(b), after],
                         r.own_ms.at[0], r.own_mr.at[b], left)

        def rel_p(b):
            return to_tp(r.h.at[phalf(b, 0), before], r.h.at[phalf(b, 0), far_side],
                         r.rel_ps.at[0], r.rel_pr.at[b], right)

        def rel_m(b):
            return to_tp(r.h.at[phalf(b, 1), after], r.h.at[phalf(b, 1), far_side],
                         r.rel_ms.at[0], r.rel_mr.at[b], left)

        def got(view, sem):
            pltpu.make_async_copy(view, view, sem).wait()

        first[1].wait()
        tails = [
            to_tp(r.tail.at[:, own], r.tail.at[:, lanes], r.tail_s.at[0], r.tail_r.at[0], q)
            for lanes, q in ((before, right), (after, left), (far_side, opp))
        ]
        for c in tails:
            c.start()
        first[0].wait()
        for b in range(2):
            own_p(b).start()
            own_m(b).start()
        for c in weights:
            c.start()

        r.ws[...] = jnp.zeros_like(r.ws)
        for lanes, q in zip(slot, order):
            r.ws[:heads, lanes] = r.step_w[:, cols(q)]
        r.bias[...] = jnp.zeros_like(r.bias)
        r.bias[:, :heads] = r.step_b[...]
        r.rate[...] = jnp.zeros_like(r.rate)
        r.rate[:, :heads] = -jnp.exp(r.dlog[...])
        r.run[...] = jnp.zeros_like(r.run)
        r.state[...] = jnp.zeros_like(r.state)

        got(r.wx, r.load.at[2])
        got(r.wb, r.load.at[3])
        got(r.tail.at[:, known], r.tail_r.at[0])

        for n in range(inner // ntile):
            lanes = slice(n * ntile, (n + 1) * ntile)
            r.rimx[:, lanes] = dot(r.tail[...], r.wx[:, lanes])
        r.rimb[...] = dot(r.tail[...], r.wb[...])
        ahead = lax.rem(at + 1, n_seq)
        rims = (
            to_seq(r.rimx.at[pl.ds(TAIL - RIM, RIM), :], r.xp.at[pl.ds(0, RIM), :],
                   r.rim_s.at[0], r.rim_r.at[0], ahead),
            to_seq(r.rimb.at[pl.ds(TAIL - RIM, RIM), :], r.bp.at[pl.ds(0, RIM), :],
                   r.rim_s.at[1], r.rim_r.at[1], ahead),
        )

        @pl.when(at < n_seq - 1)
        def _():
            for c in rims:
                c.start()

        @pl.when(at == 0)
        def _():
            r.xp[0:RIM, :] = jnp.zeros((RIM, inner), F32)
            r.bp[0:RIM, :] = jnp.zeros((RIM, 2 * LANES), F32)

        def times_step(lanes, mine):
            return lax.dot_general(
                r.h[mine, lanes], r.ws[:, lanes], (((1,), (1,)), ((), ())),
                preferred_element_type=F32,
            )

        def project_known(b):
            mine = prows(b)
            later = pl.ds(pl.multiple_of(b * piece + RIM, 8), piece)
            r.bp[later, :] = dot(r.h[mine, known], r.wb[known, :])
            r.sp[mine, :] = times_step(known, mine)

            for n in range(inner // ntile):
                lanes = slice(n * ntile, (n + 1) * ntile)
                r.xp[later, lanes] = dot(r.h[mine, known], r.wx[known, lanes])

        def project_far(b):
            mine = prows(b)
            later = pl.ds(pl.multiple_of(b * piece + RIM, 8), piece)
            r.bp[later, :] = r.bp[later, :] + dot(r.h[mine, far_side], r.wb[far_side, :])
            r.sp[mine, :] = r.sp[mine, :] + times_step(far_side, mine)

            for n in range(inner // ntile):
                lanes = slice(n * ntile, (n + 1) * ntile)
                r.xp[later, lanes] = r.xp[later, lanes] + dot(
                    r.h[mine, far_side], r.wx[far_side, lanes]
                )

        def project_gate(b):
            mine = pl.ds(b * (rows // 2), rows // 2)
            for n in range(inner // ntile):
                lanes = slice(n * ntile, (n + 1) * ntile)
                r.gs[mine, lanes] = half_silu(dot(r.h[mine, :], r.wg[:, lanes])).astype(BF16)

        def conv_and_state(k):
            mine = crows(k)
            window = pl.ds(pl.multiple_of(k * CHUNK, CHUNK), CHUNK + RIM)
            bc = conv_silu(r.bp[window, :], r.bcc_w[...], r.bcc_b[...])
            b_t = bc[:, :LANES].T.astype(BF16)
            c_in = bc[:, LANES:].astype(BF16)
            r.bt[...] = b_t
            r.cs[mine, :] = c_in
            down = lax.broadcasted_iota(jnp.int32, (CHUNK, CHUNK), 0)
            across = lax.broadcasted_iota(jnp.int32, (CHUNK, CHUNK), 1)
            lower = jnp.where(down >= across, 1.0, 0.0).astype(BF16)
            step = softplus(r.sp[mine, :] + r.bias[...])
            cum = running_sum(lower, step * r.rate[...])
            end = cum[CHUNK - 1 :, :]
            rest = jnp.exp(end - cum) * step
            r.cum[...] = cum
            r.cd[mine, :] = cum + r.run[...]
            r.run[...] = r.run[...] + end
            r.yi[...] = dot(c_in, r.state[...].astype(BF16))
            low = lax.broadcasted_iota(jnp.int32, (CHUNK, LANES), 1) < HEAD
            ends = jnp.exp(end)
            for k2 in range(pairs):
                lanes = slice(k2 * LANES, (k2 + 1) * LANES)
                x = conv_silu(r.xp[window, lanes], r.conv_w[:, lanes], r.conv_b[k2 : k2 + 1, :])
                x_step = x * pair_of(step, k2, CHUNK)[2]
                r.xw[:, lanes] = (x * pair_of(rest, k2, CHUNK)[2]).astype(BF16)
                r.dexp[:, lanes] = pair_of(ends, k2, 1)[2]
                r.xc[:, lanes] = x.astype(BF16)
                r.fed[:CHUNK, lanes] = jnp.where(low, x_step, 0.0).astype(BF16)
                r.fed[CHUNK:, lanes] = jnp.where(low, 0.0, x_step).astype(BF16)
            r.state[...] = r.dexp[...] * r.state[...] + dot(b_t, r.xw[...])

        def within(k):
            mine = crows(k)
            down = lax.broadcasted_iota(jnp.int32, (CHUNK, CHUNK), 0)
            across = lax.broadcasted_iota(jnp.int32, (CHUNK, CHUNK), 1)
            scores = jnp.where(down >= across, dot(r.cs[mine, :], r.bt[...]), 0.0)
            cum = r.cum[...]
            cum_t = cum.T
            for k2 in range(pairs):
                lanes = slice(k2 * LANES, (k2 + 1) * LANES)
                first, second, both = pair_of(cum, k2, CHUNK)
                rise = [
                    (scores * jnp.exp(jnp.minimum(v - cum_t[2 * k2 + i : 2 * k2 + i + 1, :], 0.0)))
                    .astype(BF16)
                    for i, v in enumerate((first, second))
                ]
                kept = pair_of(r.skip[...], k2, 1)[2]
                y = dot(jnp.concatenate(rise, axis=1), r.fed[:, lanes])
                r.ys[mine, lanes] = (
                    y + jnp.exp(both) * r.yi[:, lanes] + kept * r.xc[:, lanes].astype(F32)
                )

        n_y, n_x, n_c = split
        y, x, core = at // (n_x * n_c), lax.rem(at // n_c, n_x), lax.rem(at, n_c)
        apart = sorted(
            ((dy, dx, dc) for dy in range(n_y) for dx in range(n_x) for dc in range(n_c)),
            key=lambda d: (-min(d[0], n_y - d[0]) - min(d[1], n_x - d[1]), -d[2]),
        )[:-1]

        def seq_of(d):
            py = lax.rem(y + d[0], n_y)
            px = lax.rem(x + d[1], n_x)
            return (py * n_x + px) * n_c + lax.rem(core + d[2], n_c)

        def send_states():
            for k2 in range(pairs):
                lanes = slice(k2 * LANES, (k2 + 1) * LANES)
                r.dexp[:, lanes] = jnp.exp(pair_of(r.run[...], k2, 1)[2])
            for j in range(lane_parts):
                r.dtx[j] = r.dexp[:, j * slice_lanes : (j + 1) * slice_lanes]
            for j in range(n_seq):
                top = (j // lane_parts) * slice_rows
                lane = (j % lane_parts) * slice_lanes
                r.stx[j] = r.state[top : top + slice_rows, lane : lane + slice_lanes].astype(BF16)
            for d in apart:
                q = seq_of(d)
                to_seq(r.dtx.at[lax.rem(q, lane_parts)], r.drx.at[at],
                       r.dc_s.at[0], r.dc_r.at[0], q).start()
                to_seq(r.stx.at[q], r.srx.at[at], r.st_s.at[0], r.st_r.at[0], q).start()

        def gather_step(b, _):
            @pl.when(b < pieces)
            def _():
                got(r.h.at[prows(b), before], r.own_pr.at[b])
                rel_p(b).start()
                got(r.h.at[prows(b), after], r.own_mr.at[b])
                rel_m(b).start()

                @pl.when(b + 2 < pieces)
                def _():
                    own_p(b + 2).start()
                    own_m(b + 2).start()

                project_known(b)

            @pl.when(b == 1)
            def _():
                @pl.when(at > 0)
                def _():
                    got(r.xp.at[pl.ds(0, RIM), :], r.rim_r.at[0])
                    got(r.bp.at[pl.ds(0, RIM), :], r.rim_r.at[1])

            @pl.when(b > 0)
            def _():
                done = b - 1
                got(r.h.at[phalf(done, 0), far_side], r.rel_pr.at[done])
                got(r.h.at[phalf(done, 1), far_side], r.rel_mr.at[done])
                project_far(done)
                conv_and_state(done)

                @pl.when(b == pieces)
                def _():
                    send_states()

                within(done)

            return 0

        lax.fori_loop(0, pieces + 1, gather_step, 0)
        r.srx[at] = r.stx[at]
        r.drx[at] = r.dtx[lax.rem(at, lane_parts)]
        others = pl.ds(0, n_seq - 1)
        got(r.wg, r.load.at[4])
        project_gate(0)
        got(r.drx.at[others], r.dc_r.at[0])
        got(r.srx.at[others], r.st_r.at[0])

        def scan(j, before):
            r.ptx[j] = before.astype(BF16)
            return r.drx[j] * before + r.srx[j].astype(F32)

        lax.fori_loop(0, n_seq, scan, jnp.zeros((slice_rows, slice_lanes), F32))

        for d in apart:
            q = seq_of(d)
            to_seq(r.ptx.at[q], r.prx.at[at], r.pf_s.at[0], r.pf_r.at[0], q).start()
        r.prx[at] = r.ptx[at]
        project_gate(1)
        got(r.prx.at[others], r.pf_r.at[0])
        for j in range(n_seq):
            top = (j // lane_parts) * slice_rows
            lane = (j % lane_parts) * slice_lanes
            r.sin[top : top + slice_rows, lane : lane + slice_lanes] = r.prx[j].astype(F32)

        def stat_to(k, off):
            here = r.stat.at[me, k]
            return to_tp(here, here, r.sa_s.at[0], r.sa_r.at[k], lax.rem(me + off, n_tp))

        def gate(k, _):
            mine = crows(k)
            r.yi[...] = dot(r.cs[mine, :], r.sin[...].astype(BF16))
            reach = r.cd[mine, :]
            squares = jnp.zeros((CHUNK, LANES), F32)
            tops = jnp.zeros((CHUNK, LANES), F32)
            for k2 in range(pairs):
                lanes = slice(k2 * LANES, (k2 + 1) * LANES)
                _, _, both = pair_of(reach, k2, CHUNK)
                out = r.ys[mine, lanes] + jnp.exp(both) * r.yi[:, lanes]
                gated = out * r.gs[mine, lanes].astype(F32)
                squares = squares + gated * gated
                gained = gated * r.gain[k2 : k2 + 1, :]
                tops = jnp.maximum(tops, jnp.abs(gained))
                r.ys[mine, lanes] = gained
            r.stat[me, k, 0:1, :] = jnp.sum(squares.T, axis=0, keepdims=True)
            r.stat[me, k, 1:2, :] = jnp.max(tops.T, axis=0, keepdims=True)
            for off in range(1, n_tp):
                stat_to(k, off).start()
            return 0

        most = r.hist[0]
        for i in range(1, r.hist.shape[0]):
            most = jnp.maximum(most, r.hist[i])
        unscale = jnp.full((1, LANES), most, F32) / QMAX
        scale = QMAX / jnp.full((1, LANES), most, F32)
        r.peak[...] = jnp.zeros_like(r.peak)
        got(r.wo, r.load.at[5])

        def norm(k):
            mine = crows(k)
            got(r.stat.at[pl.ds(0, n_tp - 1), k], r.sa_r.at[k])
            squares = r.stat[0, k, 0:1, :]
            tops = r.stat[0, k, 1:2, :]
            for q in range(1, n_tp):
                squares = squares + r.stat[q, k, 0:1, :]
                tops = jnp.maximum(tops, r.stat[q, k, 1:2, :])
            inv = lax.rsqrt(squares * (1.0 / (inner * n_tp)) + EPS)
            r.peak[...] = jnp.maximum(r.peak[...], tops * inv)
            factor = jnp.broadcast_to(inv * scale, (CHUNK, LANES)).T
            for k2 in range(pairs):
                lanes = slice(k2 * LANES, (k2 + 1) * LANES)
                r.gs[mine, lanes] = jnp.clip(r.ys[mine, lanes] * factor, -QMAX, QMAX).astype(BF16)

        def khalf(k, side):
            return pl.ds(pl.multiple_of(k * CHUNK + side * (CHUNK // 2), CHUNK // 2), CHUNK // 2)

        def kept_half(k):
            return pl.ds(pl.multiple_of(k * (CHUNK // 2), CHUNK // 2), CHUNK // 2)

        def far_p(k):
            return to_tp(r.tr.at[khalf(k, 0), :], r.rl.at[kept_half(k), :],
                         r.far_ps.at[0], r.far_pr.at[k], right)

        def far_m(k):
            return to_tp(r.tr.at[khalf(k, 1), :], r.rr.at[kept_half(k), :],
                         r.far_ms.at[0], r.far_mr.at[k], left)

        def near_p(b):
            return to_tp(r.txp.at[brows(b), :], r.rxp.at[brows(b), :],
                         r.near_ps.at[0], r.near_pr.at[b], right)

        def near_m(b):
            return to_tp(r.txm.at[brows(b), :], r.rxm.at[brows(b), :],
                         r.near_ms.at[0], r.near_mr.at[b], left)

        lag = min(4, chunks)

        def far(k, _):
            @pl.when(k < chunks)
            def _():
                gate(k, 0)

            @pl.when(k >= lag)
            def _():
                ready = k - lag
                norm(ready)
                mine = crows(ready)
                r.tr[mine, :] = dot(r.gs[mine, :], r.wo[:, cols(opp)]).astype(BF16)
                far_p(ready).start()
                far_m(ready).start()

            return 0

        lax.fori_loop(0, chunks + lag, far, 0)
        r.pkt[...] = r.peak[...]

        def peak_to(off):
            q = lax.rem(at + off, n_seq)
            return to_seq(r.pkt, r.pkr.at[at], r.pk_s.at[0], r.pk_r.at[0], q)

        def peak_send(off, _):
            peak_to(off).start()
            return 0

        lax.fori_loop(1, n_seq, peak_send, 0)
        r.pkr[at] = r.peak[...]

        def near(b, _):
            mine = brows(b)
            r.txp[mine, :] = dot(r.gs[mine, :], r.wo[:, cols(right)]).astype(BF16)
            r.txm[mine, :] = dot(r.gs[mine, :], r.wo[:, cols(left)]).astype(BF16)
            for j in range(per):
                k = b * per + j
                top = khalf(k, 0)
                got(r.rl.at[kept_half(k), :], r.far_pr.at[k])
                r.txp[top, :] = (
                    r.txp[top, :].astype(F32) + r.rl[kept_half(k), :].astype(F32)
                ).astype(BF16)
            near_p(b).start()
            for j in range(per):
                k = b * per + j
                low = khalf(k, 1)
                got(r.rr.at[kept_half(k), :], r.far_mr.at[k])
                r.txm[low, :] = (
                    r.txm[low, :].astype(F32) + r.rr[kept_half(k), :].astype(F32)
                ).astype(BF16)
            near_m(b).start()
            return 0

        lax.fori_loop(0, blocks, near, 0)

        def finish(b, _):
            mine = brows(b)
            total = dot(r.gs[mine, :], r.wo[:, cols(me)])
            got(r.rxp.at[mine, :], r.near_pr.at[b])
            got(r.rxm.at[mine, :], r.near_mr.at[b])
            total = total + (r.rxp[mine, :].astype(F32) + r.rxm[mine, :].astype(F32))
            r.mixed[mine, :] = (total * unscale[0:1, 0:1]).astype(BF16)
            return 0

        lax.fori_loop(0, blocks, finish, 0)

        got(r.pkr.at[others], r.pk_r.at[0])
        top = lax.fori_loop(0, n_seq, lambda j, v: jnp.maximum(v, r.pkr[j]), r.peak[...])
        lane = lax.broadcasted_iota(jnp.int32, r.news.shape, 1)
        news = jnp.broadcast_to(jnp.max(top, axis=1, keepdims=True), r.news.shape)
        for i in range(1, r.hist.shape[0]):
            news = jnp.where(lane == i, r.hist[i - 1], news)
        r.news[...] = news

        got(r.tail.at[:, known], r.tail_s.at[0])

        @pl.when(at < n_seq - 1)
        def _():
            for c in rims:
                c.wait_send()

        half_own = r.h.at[pl.ds(0, rows // 2), own]
        for view, sem in (
            (r.h.at[:, own], r.own_ps), (r.h.at[:, own], r.own_ms),
            (half_own, r.rel_ps), (half_own, r.rel_ms),
            (r.rl, r.far_ps), (r.rr, r.far_ms), (r.txp, r.near_ps), (r.txm, r.near_ms),
            (r.drx.at[others], r.dc_s), (r.srx.at[others], r.st_s),
            (r.prx.at[others], r.pf_s), (r.pkr.at[others], r.pk_s),
            (r.stat.at[pl.ds(0, n_tp - 1)], r.sa_s),
        ):
            got(view, sem.at[0])

    hbm = pl.BlockSpec(memory_space=pl.ANY)
    local = pl.BlockSpec(memory_space=pltpu.VMEM)
    scalars = pl.BlockSpec(memory_space=pltpu.SMEM)
    return pl.pallas_call(
        kernel,
        name="layer",
        out_shape=(
            pltpu.VMEM((rows, part), BF16),
            pltpu.VMEM((1, 16), F32),
        ),
        in_specs=[hbm] * 4 + [local] * 9 + [hbm, scalars],
        out_specs=(local, local),
        scratch_shapes=[pltpu.VMEM(*v) for v in vmem.values()]
        + [pltpu.SemaphoreType.DMA((n,)) for n in dma.values()],
        compiler_params=pltpu.CompilerParams(
            collective_id=0, has_side_effects=True, vmem_limit_bytes=65_650_000
        ),
    )


def solution(mesh):
    n_seq, n_tp = mesh.shape["seq"], mesh.shape["tp"]
    side = max(k for k in range(1, n_seq) if 2 * k * k <= n_seq and n_seq % (2 * k) == 0)
    split = (n_seq // (2 * side), side, 2)

    def shards(
        hidden, gate_proj, input_proj, bc_proj, step_proj, step_bias, decay_log, conv_weight,
        conv_bias, bc_conv_weight, bc_conv_bias, skip_gain, norm_gain, out_proj, amax_history,
    ):
        rows, part = hidden.shape
        call = build(rows, part, gate_proj.shape[1], n_tp, n_seq, step_proj.shape[1], split)
        mixed, news = call(
            hidden, gate_proj, input_proj, bc_proj, step_proj.T, step_bias[None], decay_log[None],
            conv_weight, conv_bias.reshape(-1, LANES), bc_conv_weight, bc_conv_bias[None],
            skip_gain[None], norm_gain.reshape(-1, LANES), out_proj, amax_history,
        )
        return mixed, news.reshape(-1)

    cols = P(None, "tp")
    flat = P("tp")
    in_specs = (
        P("seq", "tp"), cols, cols, P(), cols, flat, flat, cols, flat, P(), P(), flat, flat,
        P("tp", None), P(),
    )
    return jax.shard_map(
        shards, mesh=mesh, in_specs=in_specs, out_specs=(P("seq", "tp"), P()), check_vma=False
    )
```

```python
import types

import jax
import jax.numpy as jnp
from jax import lax
from jax.experimental import pallas as pl
from jax.experimental.pallas import tpu as pltpu
from jax.sharding import PartitionSpec as P

QMAX = 448.0
EPS = 1e-05
HEAD = 64
LANES = 128
CHUNK = 128
RIM = 8
TAIL = 16
MESH = pl.DeviceIdType.MESH
F32 = jnp.float32
BF16 = jnp.bfloat16


def dot(a, b):
    return jnp.dot(a, b, preferred_element_type=F32)


def half_silu(v):
    half = 0.5 * v
    return half + half * jnp.tanh(half)


def softplus(v):
    u = jnp.exp(-jnp.abs(v))
    s = u / (2.0 + u)
    q = s * s
    series = jnp.full_like(q, 1.0 / 15.0)
    for k in (13, 11, 9, 7, 5, 3, 1):
        series = series * q + 1.0 / k
    return jnp.maximum(v, 0.0) + 2.0 * s * series


def conv_silu(window, weight, shift):
    total = shift + weight[3:4] * window[RIM:]
    for k in range(3):
        total = total + weight[k : k + 1] * pltpu.roll(window, 3 - k, 0)[RIM:]
    return half_silu(total)


def running_sum(lower, v):
    top = v.astype(BF16)
    rest = v - top.astype(F32)
    middle = rest.astype(BF16)
    last = (rest - middle.astype(F32)).astype(BF16)
    return dot(lower, top) + (dot(lower, middle) + dot(lower, last))


def pair_of(v, k, rows):
    low = lax.broadcasted_iota(jnp.int32, (rows, LANES), 1) < HEAD
    first = jnp.broadcast_to(v[:, 2 * k : 2 * k + 1], (rows, LANES))
    second = jnp.broadcast_to(v[:, 2 * k + 1 : 2 * k + 2], (rows, LANES))
    return first, second, jnp.where(low, first, second)


def build(rows, part, inner, n_tp, n_seq, heads, split):
    depth = part * n_tp
    pairs = heads // 2
    block = 256
    blocks = rows // block
    half = block // 2
    chunks = rows // CHUNK
    per = block // CHUNK
    piece = 128
    pieces = rows // piece
    most_depth = 3 * part
    half_rows = rows // 2
    hp = pieces // 2
    scan_at = min(pieces, hp + 3)
    hc = chunks // 2
    half_blocks = blocks // 2
    n_y, n_x, n_c = split
    wide = n_x * n_c
    first_near = hc - 1
    held = max(first_near - 2, 0)
    slice_rows = max(8, LANES // n_seq)
    lane_parts = n_seq * slice_rows // LANES
    slice_lanes = inner // lane_parts
    ntile = 256

    vmem = {
        "h": ((rows, depth), BF16),
        "tail": ((2 * TAIL, depth), BF16),
        "swap": ((rows // 2, part), BF16),
        "otx": ((rows // 2, part), BF16),
        "orx": ((rows // 2, part), BF16),
        "wg": ((depth, inner), BF16),
        "wx": ((depth, inner), BF16),
        "wb": ((depth, 2 * LANES), BF16),
        "ws": ((LANES, depth), BF16),
        "wo": ((inner, depth), BF16),
        "xp": ((rows + 2 * RIM, inner), F32),
        "bp": ((rows + 2 * RIM, 2 * LANES), F32),
        "sp": ((rows, LANES), F32),
        "gs": ((rows, inner), BF16),
        "ys": ((rows, inner), F32),
        "cs": ((rows, LANES), BF16),
        "cd": ((rows, LANES), F32),
        "yi": ((CHUNK, inner), F32),
        "xw": ((CHUNK, inner), BF16),
        "yg": ((CHUNK, inner), F32),
        "xc": ((CHUNK, inner), BF16),
        "fed": ((2 * CHUNK, inner), BF16),
        "bt": ((LANES, CHUNK), BF16),
        "cum": ((CHUNK, LANES), F32),
        "state": ((2, LANES, inner), F32),
        "dexp": ((1, inner), F32),
        "run": ((2, 1, LANES), F32),
        "carry": ((slice_rows, slice_lanes), F32),
        "bias": ((1, LANES), F32),
        "rate": ((1, LANES), F32),
        "stx": ((2, n_seq, slice_rows, slice_lanes), BF16),
        "srx": ((2, n_seq, slice_rows, slice_lanes), BF16),
        "ptx": ((2, n_seq, slice_rows, slice_lanes), BF16),
        "prx": ((2, n_seq, slice_rows, slice_lanes), BF16),
        "dtx": ((2, lane_parts, 1, slice_lanes), F32),
        "drx": ((2, n_seq, 1, slice_lanes), F32),
        "sin": ((LANES, inner), F32),
        "stat": ((n_tp, chunks, 8, LANES), F32),
        "tr": ((rows, part), BF16),
        "rl": ((rows // 2, part), BF16),
        "rr": ((rows // 2, part), BF16),
        "txp": ((rows, part), BF16),
        "txm": ((rows, part), BF16),
        "rxp": ((rows, part), BF16),
        "rxm": ((rows, part), BF16),
        "peak": ((1, LANES), F32),
        "pkt": ((1, LANES), F32),
        "pkr": ((n_seq, 1, LANES), F32),
    }
    small = {
        "step_w": ((heads, depth), BF16),
        "step_b": ((1, heads), F32),
        "dlog": ((1, heads), F32),
        "conv_w": ((4, inner), F32),
        "conv_b": ((inner // LANES, LANES), F32),
        "bcc_w": ((4, 2 * LANES), F32),
        "bcc_b": ((1, 2 * LANES), F32),
        "skip": ((1, heads), F32),
        "gain": ((inner // LANES, LANES), F32),
    }
    dma = {
        "smalls": len(small),
        "load": 6,
        "own_ps": 1, "own_ms": 1, "own_pr": pieces, "own_mr": pieces,
        "rel_ps": 1, "rel_ms": 1, "rel_pr": pieces, "rel_mr": pieces,
        "tail_s": 1, "tail_r": 1, "rim_s": 2, "rim_r": 2,
        "swap_s": 1, "swap_r": hp, "out_s": 1, "out_r": hc,
        "st_s": 2, "st_r": 2, "dc_s": 2, "dc_r": 2,
        "pf_s": 2, "pf_r": 2, "pk_s": 1, "pk_r": 1,
        "sa_s": 1, "sa_r": chunks,
        "far_ps": 1, "far_ms": 1, "far_pr": chunks, "far_mr": chunks,
        "near_ps": 1, "near_ms": 1, "near_pr": chunks, "near_mr": chunks,
    }
    inputs = (
        "hidden", "gate_w", "in_w", "bc_w", *(k + "_in" for k in small), "out_w", "hist",
    )
    outputs = ("mixed", "news")
    names = (*inputs, *outputs, *vmem, *small, *dma)

    def kernel(*refs):
        r = types.SimpleNamespace(**dict(zip(names, refs)))
        me = lax.axis_index("tp")
        at = lax.axis_index("seq")
        right = lax.rem(me + 1, n_tp)
        left = lax.rem(me + n_tp - 1, n_tp)
        opp = lax.rem(me + 2, n_tp)
        late = at // (n_seq // 2)

        def mate_of(q):
            return (n_y - 1 - q // wide) * wide + lax.rem(q, wide)

        mate = mate_of(at)
        home = pl.multiple_of(late * half_rows, half_rows)

        def cols(q):
            return pl.ds(pl.multiple_of(q * part, LANES), part)

        def brows(b):
            return pl.ds(pl.multiple_of(b * block, block), block)

        def crows(k):
            return pl.ds(pl.multiple_of(k * CHUNK, CHUNK), CHUNK)

        def to_tp(src, dst, send, recv, q):
            return pltpu.make_async_remote_copy(
                src_ref=src, dst_ref=dst, send_sem=send, recv_sem=recv,
                device_id={"tp": q}, device_id_type=MESH,
            )

        def to_seq(src, dst, send, recv, q):
            return pltpu.make_async_remote_copy(
                src_ref=src, dst_ref=dst, send_sem=send, recv_sem=recv,
                device_id={"seq": q}, device_id_type=MESH,
            )

        slot = [slice(i * part, (i + 1) * part) for i in range(n_tp)]
        before, own, after, far_side = slot
        known = slice(0, most_depth)
        order = (left, me, right, opp)

        def load(src, dst, i):
            return pltpu.make_async_copy(src, dst, r.load.at[i])

        first = [
            load(r.hidden.at[pl.ds(0, half_rows), :], r.h.at[pl.ds(home, half_rows), own], 0),
            load(r.hidden.at[pl.ds(half_rows, half_rows), :], r.swap, 1),
        ]
        for c in first:
            c.start()

        def by_rows(src, dst, i):
            return [
                load(src.at[pl.ds(pl.multiple_of(q * part, LANES), part), :],
                     dst.at[pl.ds(j * part, part), :], i)
                for j, q in enumerate(order)
            ]

        weights = (
            by_rows(r.in_w, r.wx, 2) + by_rows(r.bc_w, r.wb, 3) + by_rows(r.gate_w, r.wg, 4)
            + [load(r.out_w, r.wo, 5)]
        )

        smalls = [
            pltpu.make_async_copy(getattr(r, k + "_in"), getattr(r, k), r.smalls.at[i])
            for i, k in enumerate(small)
        ]

        barrier = pltpu.get_barrier_semaphore()
        for off in range(1, n_tp):
            pl.semaphore_signal(
                barrier, inc=1, device_id={"tp": lax.rem(me + off, n_tp)}, device_id_type=MESH
            )

        def greet(off, _):
            pl.semaphore_signal(
                barrier, inc=1, device_id={"seq": lax.rem(at + off, n_seq)}, device_id_type=MESH
            )
            return 0

        lax.fori_loop(1, n_seq, greet, 0)
        pl.semaphore_wait(barrier, n_tp - 1 + n_seq - 1)

        def prows(b):
            return pl.ds(pl.multiple_of(b * piece, piece), piece)

        def phalf(b, side):
            return pl.ds(pl.multiple_of(b * piece + side * (piece // 2), piece // 2), piece // 2)

        def own_p(b):
            return to_tp(r.h.at[prows(b), own], r.h.at[prows(b), before],
                         r.own_ps.at[0], r.own_pr.at[b], right)

        def own_m(b):
            return to_tp(r.h.at[prows(b), own], r.h.at[prows(b), after],
                         r.own_ms.at[0], r.own_mr.at[b], left)

        def rel_p(b):
            return to_tp(r.h.at[phalf(b, 0), before], r.h.at[phalf(b, 0), far_side],
                         r.rel_ps.at[0], r.rel_pr.at[b], right)

        def rel_m(b):
            return to_tp(r.h.at[phalf(b, 1), after], r.h.at[phalf(b, 1), far_side],
                         r.rel_ms.at[0], r.rel_mr.at[b], left)

        def got(view, sem):
            pltpu.make_async_copy(view, view, sem).wait()

        def place(i):
            zero = (pieces - i) // pieces
            low = (hp - i + pieces) // pieces
            return i + late * (zero * hp - (low - zero))

        def send_own(i):
            b = place(i)

            @pl.when(b // hp != late)
            def _():
                got(r.h.at[prows(b), own], r.swap_r.at[lax.rem(b, hp)])

            own_p(b).start()
            own_m(b).start()

        def swap(j):
            here = pl.ds(j * piece, piece)
            there = pl.ds(pl.multiple_of(late * half_rows + j * piece, piece), piece)
            return to_seq(r.swap.at[here, :], r.h.at[there, own],
                          r.swap_s.at[0], r.swap_r.at[j], mate)

        ahead = lax.rem(at + 1, n_seq)
        theirs = (ahead // (n_seq // 2)) * TAIL
        rims = (
            to_seq(r.swap.at[pl.ds(half_rows - TAIL, TAIL), :],
                   r.tail.at[pl.ds(pl.multiple_of(theirs, TAIL), TAIL), own],
                   r.rim_s.at[0], r.rim_r.at[0], ahead),
            to_seq(r.h.at[pl.ds(pl.multiple_of(home + half_rows - TAIL, TAIL), TAIL), own],
                   r.tail.at[pl.ds(pl.multiple_of(late * TAIL, TAIL), TAIL), own],
                   r.rim_s.at[1], r.rim_r.at[1], mate),
        )
        first[1].wait()

        @pl.when(at < n_seq - 1)
        def _():
            rims[0].start()

        first[0].wait()
        rims[1].start()
        send_own(0)

        @pl.when(late == 0)
        def _():
            send_own(1)

        for j in range(hp):
            swap(j).start()
        for c in (*smalls, *weights):
            c.start()
        for c in smalls:
            c.wait()

        r.ws[...] = jnp.zeros_like(r.ws)
        for lanes, q in zip(slot, order):
            r.ws[:heads, lanes] = r.step_w[:, cols(q)]
        r.bias[...] = jnp.zeros_like(r.bias)
        r.bias[:, :heads] = r.step_b[...]
        r.rate[...] = jnp.zeros_like(r.rate)
        r.rate[:, :heads] = -jnp.exp(r.dlog[...])
        r.run[...] = jnp.zeros_like(r.run)
        r.state[...] = jnp.zeros_like(r.state)
        r.carry[...] = jnp.zeros_like(r.carry)

        @pl.when(at == 0)
        def _():
            r.tail[0:TAIL, own] = jnp.zeros((TAIL, part), BF16)

        @pl.when(at > 0)
        def _():
            got(r.tail.at[pl.ds(0, TAIL), own], r.rim_r.at[0])

        got(r.tail.at[pl.ds(0, TAIL), own], r.rim_r.at[1])
        for lanes, q in ((before, right), (after, left), (far_side, opp)):
            to_tp(r.tail.at[:, own], r.tail.at[:, lanes], r.tail_s.at[0], r.tail_r.at[0], q).start()

        @pl.when(late == 1)
        def _():
            send_own(1)

        def project_rims():
            got(r.tail.at[:, known], r.tail_r.at[0])
            spots = ((0, TAIL - RIM), (half_rows + RIM, 2 * TAIL - RIM))
            for n in range(inner // ntile):
                lanes = slice(n * ntile, (n + 1) * ntile)
                ahead_x = dot(r.tail[...], r.wx[:, lanes])
                for to, row in spots:
                    r.xp[to : to + RIM, lanes] = ahead_x[row : row + RIM, :]
            ahead_b = dot(r.tail[...], r.wb[...])
            for to, row in spots:
                r.bp[to : to + RIM, :] = ahead_b[row : row + RIM, :]

        def padded(b):
            return pl.ds(pl.multiple_of(b * piece + RIM + (b // hp) * RIM, RIM), piece)

        def times_step(lanes, mine):
            return lax.dot_general(
                r.h[mine, lanes], r.ws[:, lanes], (((1,), (1,)), ((), ())),
                preferred_element_type=F32,
            )

        def project_known(b):
            mine = prows(b)
            later = padded(b)
            r.bp[later, :] = dot(r.h[mine, known], r.wb[known, :])
            r.sp[mine, :] = times_step(known, mine)

            for n in range(inner // ntile):
                lanes = slice(n * ntile, (n + 1) * ntile)
                r.xp[later, lanes] = dot(r.h[mine, known], r.wx[known, lanes])

        def project_far(b):
            mine = prows(b)
            later = padded(b)
            r.bp[later, :] = r.bp[later, :] + dot(r.h[mine, far_side], r.wb[far_side, :])
            r.sp[mine, :] = r.sp[mine, :] + times_step(far_side, mine)

            for n in range(inner // ntile):
                lanes = slice(n * ntile, (n + 1) * ntile)
                r.xp[later, lanes] = r.xp[later, lanes] + dot(
                    r.h[mine, far_side], r.wx[far_side, lanes]
                )

        def project_gate(b):
            mine = brows(b)
            for n in range(inner // ntile):
                lanes = slice(n * ntile, (n + 1) * ntile)
                r.gs[mine, lanes] = half_silu(dot(r.h[mine, :], r.wg[:, lanes])).astype(BF16)

        def conv_and_state(k):
            mine = crows(k)
            seg = k // hc
            window = pl.ds(pl.multiple_of(k * CHUNK + seg * RIM, RIM), CHUNK + RIM)
            bc = conv_silu(r.bp[window, :], r.bcc_w[...], r.bcc_b[...])
            b_t = bc[:, :LANES].T.astype(BF16)
            c_in = bc[:, LANES:].astype(BF16)
            r.bt[...] = b_t
            r.cs[mine, :] = c_in
            down = lax.broadcasted_iota(jnp.int32, (CHUNK, CHUNK), 0)
            across = lax.broadcasted_iota(jnp.int32, (CHUNK, CHUNK), 1)
            lower = jnp.where(down >= across, 1.0, 0.0).astype(BF16)
            step = softplus(r.sp[mine, :] + r.bias[...])
            cum = running_sum(lower, step * r.rate[...])
            end = cum[CHUNK - 1 :, :]
            rest = jnp.exp(end - cum) * step
            r.cum[...] = cum
            r.cd[mine, :] = cum + r.run[seg]
            r.run[seg] = r.run[seg] + end
            r.yi[...] = dot(c_in, r.state[seg].astype(BF16))
            low = lax.broadcasted_iota(jnp.int32, (CHUNK, LANES), 1) < HEAD
            ends = jnp.exp(end)
            for k2 in range(pairs):
                lanes = slice(k2 * LANES, (k2 + 1) * LANES)
                x = conv_silu(r.xp[window, lanes], r.conv_w[:, lanes], r.conv_b[k2 : k2 + 1, :])
                x_step = x * pair_of(step, k2, CHUNK)[2]
                r.xw[:, lanes] = (x * pair_of(rest, k2, CHUNK)[2]).astype(BF16)
                r.dexp[:, lanes] = pair_of(ends, k2, 1)[2]
                r.xc[:, lanes] = x.astype(BF16)
                r.fed[:CHUNK, lanes] = jnp.where(low, x_step, 0.0).astype(BF16)
                r.fed[CHUNK:, lanes] = jnp.where(low, 0.0, x_step).astype(BF16)
            r.state[seg] = r.dexp[...] * r.state[seg] + dot(b_t, r.xw[...])

        def within(k):
            mine = crows(k)
            down = lax.broadcasted_iota(jnp.int32, (CHUNK, CHUNK), 0)
            across = lax.broadcasted_iota(jnp.int32, (CHUNK, CHUNK), 1)
            scores = jnp.where(down >= across, dot(r.cs[mine, :], r.bt[...]), 0.0)
            cum = r.cum[...]
            cum_t = cum.T
            for k2 in range(pairs):
                lanes = slice(k2 * LANES, (k2 + 1) * LANES)
                first, second, both = pair_of(cum, k2, CHUNK)
                rise = [
                    (scores * jnp.exp(jnp.minimum(v - cum_t[2 * k2 + i : 2 * k2 + i + 1, :], 0.0)))
                    .astype(BF16)
                    for i, v in enumerate((first, second))
                ]
                kept = pair_of(r.skip[...], k2, 1)[2]
                y = dot(jnp.concatenate(rise, axis=1), r.fed[:, lanes])
                r.ys[mine, lanes] = (
                    y + jnp.exp(both) * r.yi[:, lanes] + kept * r.xc[:, lanes].astype(F32)
                )

        y, x, core = at // (n_x * n_c), lax.rem(at // n_c, n_x), lax.rem(at, n_c)
        apart = sorted(
            ((dy, dx, dc) for dy in range(n_y) for dx in range(n_x) for dc in range(n_c)),
            key=lambda d: (-min(d[0], n_y - d[0]) - min(d[1], n_x - d[1]), -d[2]),
        )[:-1]

        def seq_of(d):
            py = lax.rem(y + d[0], n_y)
            px = lax.rem(x + d[1], n_x)
            return (py * n_x + px) * n_c + lax.rem(core + d[2], n_c)

        others = pl.ds(0, n_seq - 1)

        def send_states(seg):
            for k2 in range(pairs):
                lanes = slice(k2 * LANES, (k2 + 1) * LANES)
                r.dexp[:, lanes] = jnp.exp(pair_of(r.run[seg], k2, 1)[2])
            for j in range(lane_parts):
                r.dtx[seg, j] = r.dexp[:, j * slice_lanes : (j + 1) * slice_lanes]
            for j in range(n_seq):
                top = (j // lane_parts) * slice_rows
                lane = (j % lane_parts) * slice_lanes
                r.stx[seg, j] = r.state[
                    seg, top : top + slice_rows, lane : lane + slice_lanes
                ].astype(BF16)
            for d in apart:
                q = seq_of(d)
                to_seq(r.dtx.at[seg, lax.rem(q, lane_parts)], r.drx.at[seg, at],
                       r.dc_s.at[seg], r.dc_r.at[seg], q).start()
                to_seq(r.stx.at[seg, q], r.srx.at[seg, at],
                       r.st_s.at[seg], r.st_r.at[seg], q).start()
            r.srx[seg, at] = r.stx[seg, at]
            r.drx[seg, at] = r.dtx[seg, lax.rem(at, lane_parts)]

        def send_prefixes(seg):
            got(r.drx.at[seg, others], r.dc_r.at[seg])
            got(r.srx.at[seg, others], r.st_r.at[seg])

            def scan(i, passed):
                base = seg * (n_seq // 2) + i // 2
                j = base + lax.rem(i, 2) * (mate_of(base) - base)
                r.ptx[seg, j] = passed.astype(BF16)
                return r.drx[seg, j] * passed + r.srx[seg, j].astype(F32)

            r.carry[...] = lax.fori_loop(0, n_seq, scan, r.carry[...])
            for d in apart:
                q = seq_of(d)
                to_seq(r.ptx.at[seg, q], r.prx.at[seg, at],
                       r.pf_s.at[seg], r.pf_r.at[seg], q).start()
            r.prx[seg, at] = r.ptx[seg, at]

        def take_prefixes(seg):
            got(r.prx.at[seg, others], r.pf_r.at[seg])
            for j in range(n_seq):
                top = (j // lane_parts) * slice_rows
                lane = (j % lane_parts) * slice_lanes
                r.sin[top : top + slice_rows, lane : lane + slice_lanes] = r.prx[seg, j].astype(F32)

        def stat_to(k, off):
            here = r.stat.at[me, k]
            return to_tp(here, here, r.sa_s.at[0], r.sa_r.at[k], lax.rem(me + off, n_tp))

        def gate(k, _):
            mine = crows(k)
            r.yg[...] = dot(r.cs[mine, :], r.sin[...].astype(BF16))
            reach = r.cd[mine, :]
            squares = jnp.zeros((CHUNK, LANES), F32)
            tops = jnp.zeros((CHUNK, LANES), F32)
            for k2 in range(pairs):
                lanes = slice(k2 * LANES, (k2 + 1) * LANES)
                _, _, both = pair_of(reach, k2, CHUNK)
                out = r.ys[mine, lanes] + jnp.exp(both) * r.yg[:, lanes]
                gated = out * r.gs[mine, lanes].astype(F32)
                squares = squares + gated * gated
                gained = gated * r.gain[k2 : k2 + 1, :]
                tops = jnp.maximum(tops, jnp.abs(gained))
                r.ys[mine, lanes] = gained
            r.stat[me, k, 0:1, :] = jnp.sum(squares.T, axis=0, keepdims=True)
            r.stat[me, k, 1:2, :] = jnp.max(tops.T, axis=0, keepdims=True)
            for off in range(1, n_tp):
                stat_to(k, off).start()
            return 0

        lag = hc

        def gather_step(i, _):
            @pl.when(i == hp + 2)
            def _():
                got(r.wg, r.load.at[4])
                lax.fori_loop(0, half_blocks, lambda b, _: (project_gate(b), 0)[1], 0)

            @pl.when(i < pieces)
            def _():
                b = place(i)
                got(r.h.at[prows(b), before], r.own_pr.at[b])
                rel_p(b).start()
                got(r.h.at[prows(b), after], r.own_mr.at[b])
                rel_m(b).start()

                @pl.when(i + 2 < pieces)
                def _():
                    send_own(i + 2)

            @pl.when(i == scan_at)
            def _():
                send_prefixes(0)

            @pl.when(i < pieces)
            def _():
                @pl.when(i == 0)
                def _():
                    got(r.wx, r.load.at[2])
                    got(r.wb, r.load.at[3])

                project_known(place(i))

            @pl.when(i == 1)
            def _():
                project_rims()

            @pl.when(i > 0)
            def _():
                done = place(i - 1)
                got(r.h.at[phalf(done, 0), far_side], r.rel_pr.at[done])
                got(r.h.at[phalf(done, 1), far_side], r.rel_mr.at[done])
                project_far(done)
                conv_and_state(done)

                @pl.when(lax.rem(done + 1, hp) == 0)
                def _():
                    send_states(done // hp)

                @pl.when(i < pieces)
                def _():
                    within(done)

            return 0

        lax.fori_loop(0, pieces + 1, gather_step, 0)

        most = r.hist[0]
        for i in range(1, r.hist.shape[0]):
            most = jnp.maximum(most, r.hist[i])
        unscale = jnp.full((1, LANES), most, F32) / QMAX
        scale = QMAX / jnp.full((1, LANES), most, F32)
        r.peak[...] = jnp.zeros_like(r.peak)
        got(r.wo, r.load.at[5])

        def norm(k):
            mine = crows(k)
            got(r.stat.at[pl.ds(0, n_tp - 1), k], r.sa_r.at[k])
            squares = r.stat[0, k, 0:1, :]
            tops = r.stat[0, k, 1:2, :]
            for q in range(1, n_tp):
                squares = squares + r.stat[q, k, 0:1, :]
                tops = jnp.maximum(tops, r.stat[q, k, 1:2, :])
            inv = lax.rsqrt(squares * (1.0 / (inner * n_tp)) + EPS)
            r.peak[...] = jnp.maximum(r.peak[...], tops * inv)
            factor = jnp.broadcast_to(inv * scale, (CHUNK, LANES)).T
            for k2 in range(pairs):
                lanes = slice(k2 * LANES, (k2 + 1) * LANES)
                r.gs[mine, lanes] = jnp.clip(r.ys[mine, lanes] * factor, -QMAX, QMAX).astype(BF16)

        def khalf(k, side):
            return pl.ds(pl.multiple_of(k * CHUNK + side * (CHUNK // 2), CHUNK // 2), CHUNK // 2)

        def kept_half(k):
            return pl.ds(pl.multiple_of(k * (CHUNK // 2), CHUNK // 2), CHUNK // 2)

        def far_p(k):
            return to_tp(r.tr.at[khalf(k, 0), :], r.rl.at[kept_half(k), :],
                         r.far_ps.at[0], r.far_pr.at[k], right)

        def far_m(k):
            return to_tp(r.tr.at[khalf(k, 1), :], r.rr.at[kept_half(k), :],
                         r.far_ms.at[0], r.far_mr.at[k], left)

        def near_p(k):
            return to_tp(r.txp.at[crows(k), :], r.rxp.at[crows(k), :],
                         r.near_ps.at[0], r.near_pr.at[k], right)

        def near_m(k):
            return to_tp(r.txm.at[crows(k), :], r.rxm.at[crows(k), :],
                         r.near_ms.at[0], r.near_mr.at[k], left)

        def far(k, seg):
            @pl.when((seg == 1) & (k == hc // 2))
            def _():
                lax.fori_loop(held, first_near, near, 0)

            @pl.when(k >= lag)
            def _():
                ready = seg * hc + k - lag
                norm(ready)
                mine = crows(ready)
                r.tr[mine, :] = dot(r.gs[mine, :], r.wo[:, cols(opp)]).astype(BF16)
                far_p(ready).start()
                far_m(ready).start()

            @pl.when(k < hc)
            def _():
                gate(seg * hc + k, 0)

            return seg

        def order_of(i):
            past = (i + chunks - first_near) // chunks
            end = (i + 1) // chunks
            return i + (1 - late) * (past - end * (chunks - first_near))

        def near(i, _):
            k = order_of(i)
            mine = crows(k)
            r.txp[mine, :] = dot(r.gs[mine, :], r.wo[:, cols(right)]).astype(BF16)
            r.txm[mine, :] = dot(r.gs[mine, :], r.wo[:, cols(left)]).astype(BF16)
            top = khalf(k, 0)
            got(r.rl.at[kept_half(k), :], r.far_pr.at[k])
            r.txp[top, :] = (
                r.txp[top, :].astype(F32) + r.rl[kept_half(k), :].astype(F32)
            ).astype(BF16)
            near_p(k).start()
            low = khalf(k, 1)
            got(r.rr.at[kept_half(k), :], r.far_mr.at[k])
            r.txm[low, :] = (
                r.txm[low, :].astype(F32) + r.rr[kept_half(k), :].astype(F32)
            ).astype(BF16)
            near_m(k).start()
            return 0

        def segment(seg, _):
            take_prefixes(seg)
            lax.fori_loop(0, hc + lag, far, seg)

            @pl.when(seg == 0)
            def _():
                send_prefixes(1)
                within(chunks - 1)
                lax.fori_loop(half_blocks, blocks, lambda b, _: (project_gate(b), 0)[1], 0)
                lax.fori_loop(0, held, near, 0)

            return 0

        lax.fori_loop(0, 2, segment, 0)
        r.pkt[...] = r.peak[...]

        def peak_to(off):
            q = lax.rem(at + off, n_seq)
            return to_seq(r.pkt, r.pkr.at[at], r.pk_s.at[0], r.pk_r.at[0], q)

        def peak_send(off, _):
            peak_to(off).start()
            return 0

        lax.fori_loop(1, n_seq, peak_send, 0)
        r.pkr[at] = r.peak[...]

        lax.fori_loop(first_near, chunks, near, 0)

        def back(j):
            here = pl.ds(pl.multiple_of(j * CHUNK, CHUNK), CHUNK)
            return to_seq(r.otx.at[here, :], r.orx.at[here, :],
                          r.out_s.at[0], r.out_r.at[j], mate)

        def finish(i, _):
            k = order_of(i)
            mine = crows(k)
            total = dot(r.gs[mine, :], r.wo[:, cols(me)])
            got(r.rxp.at[mine, :], r.near_pr.at[k])
            got(r.rxm.at[mine, :], r.near_mr.at[k])
            total = total + (r.rxp[mine, :].astype(F32) + r.rxm[mine, :].astype(F32))
            out = (total * unscale[0:1, 0:1]).astype(BF16)
            j = lax.rem(k, hc)
            here = pl.ds(pl.multiple_of(j * CHUNK, CHUNK), CHUNK)

            @pl.when(k // hc == late)
            def _():
                r.mixed[here, :] = out

            @pl.when(k // hc != late)
            def _():
                r.otx[here, :] = out
                back(j).start()

            return 0

        lax.fori_loop(0, chunks, finish, 0)
        for j in range(hc):
            got(r.orx.at[pl.ds(j * CHUNK, CHUNK), :], r.out_r.at[j])
            to = half_rows + j * CHUNK
            r.mixed[to : to + CHUNK, :] = r.orx[j * CHUNK : (j + 1) * CHUNK, :]
        got(r.pkr.at[others], r.pk_r.at[0])
        top = lax.fori_loop(0, n_seq, lambda j, v: jnp.maximum(v, r.pkr[j]), r.peak[...])
        lane = lax.broadcasted_iota(jnp.int32, r.news.shape, 1)
        news = jnp.broadcast_to(jnp.max(top, axis=1, keepdims=True), r.news.shape)
        for i in range(1, r.hist.shape[0]):
            news = jnp.where(lane == i, r.hist[i - 1], news)
        r.news[...] = news

        got(r.tail.at[:, known], r.tail_s.at[0])

        @pl.when(at < n_seq - 1)
        def _():
            rims[0].wait_send()

        rims[1].wait_send()
        half_own = r.h.at[pl.ds(0, rows // 2), own]
        for view, sem in (
            (r.h.at[:, own], r.own_ps), (r.h.at[:, own], r.own_ms),
            (half_own, r.rel_ps), (half_own, r.rel_ms),
            (r.rl, r.far_ps), (r.rr, r.far_ms), (r.txp, r.near_ps), (r.txm, r.near_ms),
            (r.swap, r.swap_s), (r.otx, r.out_s), (r.pkr.at[others], r.pk_s),
            (r.stat.at[pl.ds(0, n_tp - 1)], r.sa_s),
        ):
            got(view, sem.at[0])
        for seg in range(2):
            got(r.drx.at[seg, others], r.dc_s.at[seg])
            got(r.srx.at[seg, others], r.st_s.at[seg])
            got(r.prx.at[seg, others], r.pf_s.at[seg])

    hbm = pl.BlockSpec(memory_space=pl.ANY)
    local = pl.BlockSpec(memory_space=pltpu.VMEM)
    scalars = pl.BlockSpec(memory_space=pltpu.SMEM)
    return pl.pallas_call(
        kernel,
        name="layer",
        out_shape=(
            pltpu.VMEM((rows, part), BF16),
            pltpu.VMEM((1, 16), F32),
        ),
        in_specs=[hbm] * 14 + [scalars],
        out_specs=(local, local),
        scratch_shapes=[pltpu.VMEM(*v) for v in (*vmem.values(), *small.values())]
        + [pltpu.SemaphoreType.DMA((n,)) for n in dma.values()],
        compiler_params=pltpu.CompilerParams(
            collective_id=0, has_side_effects=True, vmem_limit_bytes=65_650_000
        ),
    )


def solution(mesh):
    n_seq, n_tp = mesh.shape["seq"], mesh.shape["tp"]
    side = max(k for k in range(1, n_seq) if 2 * k * k <= n_seq and n_seq % (2 * k) == 0)
    split = (n_seq // (2 * side), side, 2)

    def shards(
        hidden, gate_proj, input_proj, bc_proj, step_proj, step_bias, decay_log, conv_weight,
        conv_bias, bc_conv_weight, bc_conv_bias, skip_gain, norm_gain, out_proj, amax_history,
    ):
        rows, part = hidden.shape
        call = build(rows, part, gate_proj.shape[1], n_tp, n_seq, step_proj.shape[1], split)
        mixed, news = call(
            hidden, gate_proj, input_proj, bc_proj, step_proj.T, step_bias[None], decay_log[None],
            conv_weight, conv_bias.reshape(-1, LANES), bc_conv_weight, bc_conv_bias[None],
            skip_gain[None], norm_gain.reshape(-1, LANES), out_proj, amax_history,
        )
        return mixed, news.reshape(-1)

    cols = P(None, "tp")
    flat = P("tp")
    in_specs = (
        P("seq", "tp"), cols, cols, P(), cols, flat, flat, cols, flat, P(), P(), flat, flat,
        P("tp", None), P(),
    )
    return jax.shard_map(
        shards, mesh=mesh, in_specs=in_specs, out_specs=(P("seq", "tp"), P()), check_vma=False
    )
```

```python
import types

import jax
import jax.numpy as jnp
from jax import lax
from jax.experimental import pallas as pl
from jax.experimental.pallas import tpu as pltpu
from jax.sharding import PartitionSpec as P

QMAX = 448.0
EPS = 1e-05
HEAD = 64
LANES = 128
CHUNK = 128
RIM = 8
TAIL = 16
MESH = pl.DeviceIdType.MESH
F32 = jnp.float32
BF16 = jnp.bfloat16


def dot(a, b):
    return jnp.dot(a, b, preferred_element_type=F32)


def half_silu(v):
    half = 0.5 * v
    return half + half * jnp.tanh(half)


def softplus(v):
    u = jnp.exp(-jnp.abs(v))
    s = u / (2.0 + u)
    q = s * s
    series = jnp.full_like(q, 1.0 / 15.0)
    for k in (13, 11, 9, 7, 5, 3, 1):
        series = series * q + 1.0 / k
    return jnp.maximum(v, 0.0) + 2.0 * s * series


def conv_silu(window, weight, shift):
    total = shift + weight[3:4] * window[RIM:]
    for k in range(3):
        total = total + weight[k : k + 1] * pltpu.roll(window, 3 - k, 0)[RIM:]
    return half_silu(total)


def running_sum(lower, v):
    top = v.astype(BF16)
    rest = v - top.astype(F32)
    middle = rest.astype(BF16)
    last = (rest - middle.astype(F32)).astype(BF16)
    return dot(lower, top) + (dot(lower, middle) + dot(lower, last))


def pair_of(v, k, rows):
    low = lax.broadcasted_iota(jnp.int32, (rows, LANES), 1) < HEAD
    first = jnp.broadcast_to(v[:, 2 * k : 2 * k + 1], (rows, LANES))
    second = jnp.broadcast_to(v[:, 2 * k + 1 : 2 * k + 2], (rows, LANES))
    return first, second, jnp.where(low, first, second)


def build(rows, part, inner, n_tp, n_seq, heads, split):
    depth = part * n_tp
    pairs = heads // 2
    block = 256
    blocks = rows // block
    half = block // 2
    chunks = rows // CHUNK
    per = block // CHUNK
    piece = 128
    pieces = rows // piece
    most_depth = 3 * part
    half_rows = rows // 2
    hp = pieces // 2
    scan_at = min(pieces, hp + 3)
    hc = chunks // 2
    half_blocks = blocks // 2
    n_y, n_x, n_c = split
    wide = n_x * n_c
    first_near = hc - 1
    held = max(first_near - 2, 0)
    slice_rows = max(8, LANES // n_seq)
    lane_parts = n_seq * slice_rows // LANES
    slice_lanes = inner // lane_parts
    ntile = 256

    vmem = {
        "h": ((rows, depth), BF16),
        "tail": ((2 * TAIL, depth), BF16),
        "swap": ((rows // 2, part), BF16),
        "otx": ((rows // 2, part), BF16),
        "orx": ((rows // 2, part), BF16),
        "wg": ((depth, inner), BF16),
        "wx": ((depth, inner), BF16),
        "wb": ((depth, 2 * LANES), BF16),
        "ws": ((LANES, depth), BF16),
        "wo": ((inner, depth), BF16),
        "xp": ((rows + 2 * RIM, inner), F32),
        "bp": ((rows + 2 * RIM, 2 * LANES), F32),
        "sp": ((rows, LANES), F32),
        "gs": ((rows, inner), BF16),
        "ys": ((rows, inner), F32),
        "cs": ((rows, LANES), BF16),
        "cd": ((rows, LANES), F32),
        "yi": ((CHUNK, inner), F32),
        "xw": ((CHUNK, inner), BF16),
        "yg": ((CHUNK, inner), F32),
        "xc": ((CHUNK, inner), BF16),
        "fed": ((2 * CHUNK, inner), BF16),
        "bt": ((LANES, CHUNK), BF16),
        "cum": ((CHUNK, LANES), F32),
        "state": ((2, LANES, inner), F32),
        "dexp": ((1, inner), F32),
        "run": ((2, 1, LANES), F32),
        "carry": ((slice_rows, slice_lanes), F32),
        "bias": ((1, LANES), F32),
        "rate": ((1, LANES), F32),
        "stx": ((2, n_seq, slice_rows, slice_lanes), BF16),
        "srx": ((2, n_seq, slice_rows, slice_lanes), BF16),
        "ptx": ((2, n_seq, slice_rows, slice_lanes), BF16),
        "prx": ((2, n_seq, slice_rows, slice_lanes), BF16),
        "dtx": ((2, lane_parts, 1, slice_lanes), F32),
        "drx": ((2, n_seq, 1, slice_lanes), F32),
        "sin": ((LANES, inner), F32),
        "stat": ((n_tp, chunks, 8, LANES), F32),
        "tr": ((rows, part), BF16),
        "rl": ((rows // 2, part), BF16),
        "rr": ((rows // 2, part), BF16),
        "txp": ((rows, part), BF16),
        "txm": ((rows, part), BF16),
        "rxp": ((rows, part), BF16),
        "rxm": ((rows, part), BF16),
        "peak": ((1, LANES), F32),
        "pkt": ((1, LANES), F32),
        "pkr": ((n_seq, 1, LANES), F32),
    }
    small = {
        "step_w": ((heads, depth), BF16),
        "step_b": ((1, heads), F32),
        "dlog": ((1, heads), F32),
        "conv_w": ((4, inner), F32),
        "conv_b": ((inner // LANES, LANES), F32),
        "bcc_w": ((4, 2 * LANES), F32),
        "bcc_b": ((1, 2 * LANES), F32),
        "skip": ((1, heads), F32),
        "gain": ((inner // LANES, LANES), F32),
    }
    dma = {
        "smalls": len(small),
        "load": 6,
        "own_ps": 1, "own_ms": 1, "own_pr": pieces, "own_mr": pieces,
        "rel_ps": 1, "rel_ms": 1, "rel_pr": pieces, "rel_mr": pieces,
        "tail_s": 1, "tail_r": 1, "rim_s": 2, "rim_r": 2,
        "swap_s": 1, "swap_r": hp, "out_s": 1, "out_r": hc,
        "st_s": 2, "st_r": 2, "dc_s": 2, "dc_r": 2,
        "pf_s": 2, "pf_r": 2, "pk_s": 1, "pk_r": 1,
        "sa_s": 1, "sa_r": chunks,
        "far_ps": 1, "far_ms": 1, "far_pr": chunks, "far_mr": chunks,
        "near_ps": 1, "near_ms": 1, "near_pr": chunks, "near_mr": chunks,
    }
    inputs = (
        "hidden", "gate_w", "in_w", "bc_w", *(k + "_in" for k in small), "out_w", "hist",
    )
    outputs = ("mixed", "news")
    names = (*inputs, *outputs, *vmem, *small, *dma)

    def kernel(*refs):
        r = types.SimpleNamespace(**dict(zip(names, refs)))
        me = lax.axis_index("tp")
        at = lax.axis_index("seq")
        right = lax.rem(me + 1, n_tp)
        left = lax.rem(me + n_tp - 1, n_tp)
        opp = lax.rem(me + 2, n_tp)
        late = at // (n_seq // 2)

        def mate_of(q):
            return (n_y - 1 - q // wide) * wide + lax.rem(q, wide)

        mate = mate_of(at)
        home = pl.multiple_of(late * half_rows, half_rows)

        def cols(q):
            return pl.ds(pl.multiple_of(q * part, LANES), part)

        def brows(b):
            return pl.ds(pl.multiple_of(b * block, block), block)

        def crows(k):
            return pl.ds(pl.multiple_of(k * CHUNK, CHUNK), CHUNK)

        def to_tp(src, dst, send, recv, q):
            return pltpu.make_async_remote_copy(
                src_ref=src, dst_ref=dst, send_sem=send, recv_sem=recv,
                device_id={"tp": q}, device_id_type=MESH,
            )

        def to_seq(src, dst, send, recv, q):
            return pltpu.make_async_remote_copy(
                src_ref=src, dst_ref=dst, send_sem=send, recv_sem=recv,
                device_id={"seq": q}, device_id_type=MESH,
            )

        slot = [slice(i * part, (i + 1) * part) for i in range(n_tp)]
        before, own, after, far_side = slot
        known = slice(0, most_depth)
        order = (left, me, right, opp)

        def load(src, dst, i):
            return pltpu.make_async_copy(src, dst, r.load.at[i])

        first = [
            load(r.hidden.at[pl.ds(0, half_rows), :], r.h.at[pl.ds(home, half_rows), own], 0),
            load(r.hidden.at[pl.ds(half_rows, half_rows), :], r.swap, 1),
        ]
        for c in first:
            c.start()

        smalls = [
            pltpu.make_async_copy(getattr(r, k + "_in"), getattr(r, k), r.smalls.at[i])
            for i, k in enumerate(small)
        ]
        for c in smalls:
            c.start()

        def by_rows(src, dst, i):
            return [
                load(src.at[pl.ds(pl.multiple_of(q * part, LANES), part), :],
                     dst.at[pl.ds(j * part, part), :], i)
                for j, q in enumerate(order)
            ]

        weights = (
            by_rows(r.in_w, r.wx, 2) + by_rows(r.bc_w, r.wb, 3) + by_rows(r.gate_w, r.wg, 4)
            + [load(r.out_w, r.wo, 5)]
        )

        barrier = pltpu.get_barrier_semaphore()
        for off in range(1, n_tp):
            pl.semaphore_signal(
                barrier, inc=1, device_id={"tp": lax.rem(me + off, n_tp)}, device_id_type=MESH
            )

        def greet(off, _):
            pl.semaphore_signal(
                barrier, inc=1, device_id={"seq": lax.rem(at + off, n_seq)}, device_id_type=MESH
            )
            return 0

        lax.fori_loop(1, n_seq, greet, 0)
        pl.semaphore_wait(barrier, n_tp - 1 + n_seq - 1)

        def prows(b):
            return pl.ds(pl.multiple_of(b * piece, piece), piece)

        def phalf(b, side):
            return pl.ds(pl.multiple_of(b * piece + side * (piece // 2), piece // 2), piece // 2)

        def own_p(b):
            return to_tp(r.h.at[prows(b), own], r.h.at[prows(b), before],
                         r.own_ps.at[0], r.own_pr.at[b], right)

        def own_m(b):
            return to_tp(r.h.at[prows(b), own], r.h.at[prows(b), after],
                         r.own_ms.at[0], r.own_mr.at[b], left)

        def rel_p(b):
            return to_tp(r.h.at[phalf(b, 0), before], r.h.at[phalf(b, 0), far_side],
                         r.rel_ps.at[0], r.rel_pr.at[b], right)

        def rel_m(b):
            return to_tp(r.h.at[phalf(b, 1), after], r.h.at[phalf(b, 1), far_side],
                         r.rel_ms.at[0], r.rel_mr.at[b], left)

        def got(view, sem):
            pltpu.make_async_copy(view, view, sem).wait()

        def place(i):
            zero = (pieces - i) // pieces
            low = (hp - i + pieces) // pieces
            return i + late * (zero * hp - (low - zero))

        def send_own(i):
            b = place(i)

            @pl.when(b // hp != late)
            def _():
                got(r.h.at[prows(b), own], r.swap_r.at[lax.rem(b, hp)])

            own_p(b).start()
            own_m(b).start()

        def swap(j):
            here = pl.ds(j * piece, piece)
            there = pl.ds(pl.multiple_of(late * half_rows + j * piece, piece), piece)
            return to_seq(r.swap.at[here, :], r.h.at[there, own],
                          r.swap_s.at[0], r.swap_r.at[j], mate)

        ahead = lax.rem(at + 1, n_seq)
        theirs = (ahead // (n_seq // 2)) * TAIL
        rims = (
            to_seq(r.swap.at[pl.ds(half_rows - TAIL, TAIL), :],
                   r.tail.at[pl.ds(pl.multiple_of(theirs, TAIL), TAIL), own],
                   r.rim_s.at[0], r.rim_r.at[0], ahead),
            to_seq(r.h.at[pl.ds(pl.multiple_of(home + half_rows - TAIL, TAIL), TAIL), own],
                   r.tail.at[pl.ds(pl.multiple_of(late * TAIL, TAIL), TAIL), own],
                   r.rim_s.at[1], r.rim_r.at[1], mate),
        )
        first[1].wait()

        @pl.when(at < n_seq - 1)
        def _():
            rims[0].start()

        first[0].wait()
        rims[1].start()
        send_own(0)

        @pl.when(late == 0)
        def _():
            send_own(1)

        for j in range(hp):
            swap(j).start()
        for c in weights:
            c.start()
        for c in smalls:
            c.wait()

        r.ws[...] = jnp.zeros_like(r.ws)
        for lanes, q in zip(slot, order):
            r.ws[:heads, lanes] = r.step_w[:, cols(q)]
        r.bias[...] = jnp.zeros_like(r.bias)
        r.bias[:, :heads] = r.step_b[...]
        r.rate[...] = jnp.zeros_like(r.rate)
        r.rate[:, :heads] = -jnp.exp(r.dlog[...])
        r.run[...] = jnp.zeros_like(r.run)
        r.state[...] = jnp.zeros_like(r.state)
        r.carry[...] = jnp.zeros_like(r.carry)

        @pl.when(at == 0)
        def _():
            r.tail[0:TAIL, own] = jnp.zeros((TAIL, part), BF16)

        @pl.when(at > 0)
        def _():
            got(r.tail.at[pl.ds(0, TAIL), own], r.rim_r.at[0])

        got(r.tail.at[pl.ds(0, TAIL), own], r.rim_r.at[1])
        for lanes, q in ((before, right), (after, left), (far_side, opp)):
            to_tp(r.tail.at[:, own], r.tail.at[:, lanes], r.tail_s.at[0], r.tail_r.at[0], q).start()

        @pl.when(late == 1)
        def _():
            send_own(1)

        def project_rims():
            got(r.tail.at[:, known], r.tail_r.at[0])
            spots = ((0, TAIL - RIM), (half_rows + RIM, 2 * TAIL - RIM))
            for n in range(inner // ntile):
                lanes = slice(n * ntile, (n + 1) * ntile)
                ahead_x = dot(r.tail[...], r.wx[:, lanes])
                for to, row in spots:
                    r.xp[to : to + RIM, lanes] = ahead_x[row : row + RIM, :]
            ahead_b = dot(r.tail[...], r.wb[...])
            for to, row in spots:
                r.bp[to : to + RIM, :] = ahead_b[row : row + RIM, :]

        def padded(b):
            return pl.ds(pl.multiple_of(b * piece + RIM + (b // hp) * RIM, RIM), piece)

        def times_step(lanes, mine):
            return lax.dot_general(
                r.h[mine, lanes], r.ws[:, lanes], (((1,), (1,)), ((), ())),
                preferred_element_type=F32,
            )

        def project_known(b):
            mine = prows(b)
            later = padded(b)
            r.bp[later, :] = dot(r.h[mine, known], r.wb[known, :])
            r.sp[mine, :] = times_step(known, mine)

            for n in range(inner // ntile):
                lanes = slice(n * ntile, (n + 1) * ntile)
                r.xp[later, lanes] = dot(r.h[mine, known], r.wx[known, lanes])

        def project_far(b):
            mine = prows(b)
            later = padded(b)
            r.bp[later, :] = r.bp[later, :] + dot(r.h[mine, far_side], r.wb[far_side, :])
            r.sp[mine, :] = r.sp[mine, :] + times_step(far_side, mine)

            for n in range(inner // ntile):
                lanes = slice(n * ntile, (n + 1) * ntile)
                r.xp[later, lanes] = r.xp[later, lanes] + dot(
                    r.h[mine, far_side], r.wx[far_side, lanes]
                )

        def project_gate(b):
            mine = brows(b)
            for n in range(inner // ntile):
                lanes = slice(n * ntile, (n + 1) * ntile)
                r.gs[mine, lanes] = half_silu(dot(r.h[mine, :], r.wg[:, lanes])).astype(BF16)

        def conv_and_state(k):
            mine = crows(k)
            seg = k // hc
            window = pl.ds(pl.multiple_of(k * CHUNK + seg * RIM, RIM), CHUNK + RIM)
            bc = conv_silu(r.bp[window, :], r.bcc_w[...], r.bcc_b[...])
            b_t = bc[:, :LANES].T.astype(BF16)
            c_in = bc[:, LANES:].astype(BF16)
            r.bt[...] = b_t
            r.cs[mine, :] = c_in
            down = lax.broadcasted_iota(jnp.int32, (CHUNK, CHUNK), 0)
            across = lax.broadcasted_iota(jnp.int32, (CHUNK, CHUNK), 1)
            lower = jnp.where(down >= across, 1.0, 0.0).astype(BF16)
            step = softplus(r.sp[mine, :] + r.bias[...])
            cum = running_sum(lower, step * r.rate[...])
            end = cum[CHUNK - 1 :, :]
            rest = jnp.exp(end - cum) * step
            r.cum[...] = cum
            r.cd[mine, :] = cum + r.run[seg]
            r.run[seg] = r.run[seg] + end
            r.yi[...] = dot(c_in, r.state[seg].astype(BF16))
            low = lax.broadcasted_iota(jnp.int32, (CHUNK, LANES), 1) < HEAD
            ends = jnp.exp(end)
            for k2 in range(pairs):
                lanes = slice(k2 * LANES, (k2 + 1) * LANES)
                x = conv_silu(r.xp[window, lanes], r.conv_w[:, lanes], r.conv_b[k2 : k2 + 1, :])
                x_step = x * pair_of(step, k2, CHUNK)[2]
                r.xw[:, lanes] = (x * pair_of(rest, k2, CHUNK)[2]).astype(BF16)
                r.dexp[:, lanes] = pair_of(ends, k2, 1)[2]
                r.xc[:, lanes] = x.astype(BF16)
                r.fed[:CHUNK, lanes] = jnp.where(low, x_step, 0.0).astype(BF16)
                r.fed[CHUNK:, lanes] = jnp.where(low, 0.0, x_step).astype(BF16)
            r.state[seg] = r.dexp[...] * r.state[seg] + dot(b_t, r.xw[...])

        def within(k):
            mine = crows(k)
            down = lax.broadcasted_iota(jnp.int32, (CHUNK, CHUNK), 0)
            across = lax.broadcasted_iota(jnp.int32, (CHUNK, CHUNK), 1)
            scores = jnp.where(down >= across, dot(r.cs[mine, :], r.bt[...]), 0.0)
            cum = r.cum[...]
            cum_t = cum.T
            for k2 in range(pairs):
                lanes = slice(k2 * LANES, (k2 + 1) * LANES)
                first, second, both = pair_of(cum, k2, CHUNK)
                rise = [
                    (scores * jnp.exp(jnp.minimum(v - cum_t[2 * k2 + i : 2 * k2 + i + 1, :], 0.0)))
                    .astype(BF16)
                    for i, v in enumerate((first, second))
                ]
                kept = pair_of(r.skip[...], k2, 1)[2]
                y = dot(jnp.concatenate(rise, axis=1), r.fed[:, lanes])
                r.ys[mine, lanes] = (
                    y + jnp.exp(both) * r.yi[:, lanes] + kept * r.xc[:, lanes].astype(F32)
                )

        y, x, core = at // (n_x * n_c), lax.rem(at // n_c, n_x), lax.rem(at, n_c)
        apart = sorted(
            ((dy, dx, dc) for dy in range(n_y) for dx in range(n_x) for dc in range(n_c)),
            key=lambda d: (-min(d[0], n_y - d[0]) - min(d[1], n_x - d[1]), -d[2]),
        )[:-1]

        def seq_of(d):
            py = lax.rem(y + d[0], n_y)
            px = lax.rem(x + d[1], n_x)
            return (py * n_x + px) * n_c + lax.rem(core + d[2], n_c)

        others = pl.ds(0, n_seq - 1)

        def send_states(seg):
            for k2 in range(pairs):
                lanes = slice(k2 * LANES, (k2 + 1) * LANES)
                r.dexp[:, lanes] = jnp.exp(pair_of(r.run[seg], k2, 1)[2])
            for j in range(lane_parts):
                r.dtx[seg, j] = r.dexp[:, j * slice_lanes : (j + 1) * slice_lanes]
            for j in range(n_seq):
                top = (j // lane_parts) * slice_rows
                lane = (j % lane_parts) * slice_lanes
                r.stx[seg, j] = r.state[
                    seg, top : top + slice_rows, lane : lane + slice_lanes
                ].astype(BF16)
            for d in apart:
                q = seq_of(d)
                to_seq(r.dtx.at[seg, lax.rem(q, lane_parts)], r.drx.at[seg, at],
                       r.dc_s.at[seg], r.dc_r.at[seg], q).start()
                to_seq(r.stx.at[seg, q], r.srx.at[seg, at],
                       r.st_s.at[seg], r.st_r.at[seg], q).start()
            r.srx[seg, at] = r.stx[seg, at]
            r.drx[seg, at] = r.dtx[seg, lax.rem(at, lane_parts)]

        def send_prefixes(seg):
            got(r.drx.at[seg, others], r.dc_r.at[seg])
            got(r.srx.at[seg, others], r.st_r.at[seg])

            def scan(i, passed):
                base = seg * (n_seq // 2) + i // 2
                j = base + lax.rem(i, 2) * (mate_of(base) - base)
                r.ptx[seg, j] = passed.astype(BF16)
                return r.drx[seg, j] * passed + r.srx[seg, j].astype(F32)

            r.carry[...] = lax.fori_loop(0, n_seq, scan, r.carry[...])
            for d in apart:
                q = seq_of(d)
                to_seq(r.ptx.at[seg, q], r.prx.at[seg, at],
                       r.pf_s.at[seg], r.pf_r.at[seg], q).start()
            r.prx[seg, at] = r.ptx[seg, at]

        def take_prefixes(seg):
            got(r.prx.at[seg, others], r.pf_r.at[seg])
            for j in range(n_seq):
                top = (j // lane_parts) * slice_rows
                lane = (j % lane_parts) * slice_lanes
                r.sin[top : top + slice_rows, lane : lane + slice_lanes] = r.prx[seg, j].astype(F32)

        def stat_to(k, off):
            here = r.stat.at[me, k]
            return to_tp(here, here, r.sa_s.at[0], r.sa_r.at[k], lax.rem(me + off, n_tp))

        def gate(k, _):
            mine = crows(k)
            r.yg[...] = dot(r.cs[mine, :], r.sin[...].astype(BF16))
            reach = r.cd[mine, :]
            squares = jnp.zeros((CHUNK, LANES), F32)
            tops = jnp.zeros((CHUNK, LANES), F32)
            for k2 in range(pairs):
                lanes = slice(k2 * LANES, (k2 + 1) * LANES)
                _, _, both = pair_of(reach, k2, CHUNK)
                out = r.ys[mine, lanes] + jnp.exp(both) * r.yg[:, lanes]
                gated = out * r.gs[mine, lanes].astype(F32)
                squares = squares + gated * gated
                gained = gated * r.gain[k2 : k2 + 1, :]
                tops = jnp.maximum(tops, jnp.abs(gained))
                r.ys[mine, lanes] = gained
            r.stat[me, k, 0:1, :] = jnp.sum(squares.T, axis=0, keepdims=True)
            r.stat[me, k, 1:2, :] = jnp.max(tops.T, axis=0, keepdims=True)
            for off in range(1, n_tp):
                stat_to(k, off).start()
            return 0

        lag = hc

        def gather_step(i, _):
            @pl.when(i == hp + 2)
            def _():
                got(r.wg, r.load.at[4])
                lax.fori_loop(0, half_blocks, lambda b, _: (project_gate(b), 0)[1], 0)

            @pl.when(i < pieces)
            def _():
                b = place(i)
                got(r.h.at[prows(b), before], r.own_pr.at[b])
                rel_p(b).start()
                got(r.h.at[prows(b), after], r.own_mr.at[b])
                rel_m(b).start()

                @pl.when(i + 2 < pieces)
                def _():
                    send_own(i + 2)

            @pl.when(i == scan_at)
            def _():
                send_prefixes(0)

            @pl.when(i < pieces)
            def _():
                @pl.when(i == 0)
                def _():
                    got(r.wx, r.load.at[2])
                    got(r.wb, r.load.at[3])

                project_known(place(i))

            @pl.when(i == 1)
            def _():
                project_rims()

            @pl.when(i > 0)
            def _():
                done = place(i - 1)
                got(r.h.at[phalf(done, 0), far_side], r.rel_pr.at[done])
                got(r.h.at[phalf(done, 1), far_side], r.rel_mr.at[done])
                project_far(done)
                conv_and_state(done)

                @pl.when(lax.rem(done + 1, hp) == 0)
                def _():
                    send_states(done // hp)

                within(done)

            return 0

        lax.fori_loop(0, pieces + 1, gather_step, 0)

        most = r.hist[0]
        for i in range(1, r.hist.shape[0]):
            most = jnp.maximum(most, r.hist[i])
        unscale = jnp.full((1, LANES), most, F32) / QMAX
        scale = QMAX / jnp.full((1, LANES), most, F32)
        r.peak[...] = jnp.zeros_like(r.peak)
        got(r.wo, r.load.at[5])

        def norm(k):
            mine = crows(k)
            got(r.stat.at[pl.ds(0, n_tp - 1), k], r.sa_r.at[k])
            squares = r.stat[0, k, 0:1, :]
            tops = r.stat[0, k, 1:2, :]
            for q in range(1, n_tp):
                squares = squares + r.stat[q, k, 0:1, :]
                tops = jnp.maximum(tops, r.stat[q, k, 1:2, :])
            inv = lax.rsqrt(squares * (1.0 / (inner * n_tp)) + EPS)
            r.peak[...] = jnp.maximum(r.peak[...], tops * inv)
            factor = jnp.broadcast_to(inv * scale, (CHUNK, LANES)).T
            for k2 in range(pairs):
                lanes = slice(k2 * LANES, (k2 + 1) * LANES)
                r.gs[mine, lanes] = jnp.clip(r.ys[mine, lanes] * factor, -QMAX, QMAX).astype(BF16)

        def khalf(k, side):
            return pl.ds(pl.multiple_of(k * CHUNK + side * (CHUNK // 2), CHUNK // 2), CHUNK // 2)

        def kept_half(k):
            return pl.ds(pl.multiple_of(k * (CHUNK // 2), CHUNK // 2), CHUNK // 2)

        def far_p(k):
            return to_tp(r.tr.at[khalf(k, 0), :], r.rl.at[kept_half(k), :],
                         r.far_ps.at[0], r.far_pr.at[k], right)

        def far_m(k):
            return to_tp(r.tr.at[khalf(k, 1), :], r.rr.at[kept_half(k), :],
                         r.far_ms.at[0], r.far_mr.at[k], left)

        def near_p(k):
            return to_tp(r.txp.at[crows(k), :], r.rxp.at[crows(k), :],
                         r.near_ps.at[0], r.near_pr.at[k], right)

        def near_m(k):
            return to_tp(r.txm.at[crows(k), :], r.rxm.at[crows(k), :],
                         r.near_ms.at[0], r.near_mr.at[k], left)

        def far(k, seg):
            @pl.when((seg == 1) & (k == hc // 2))
            def _():
                lax.fori_loop(held, first_near, near, 0)

            @pl.when(k >= lag)
            def _():
                ready = seg * hc + k - lag
                norm(ready)
                mine = crows(ready)
                r.tr[mine, :] = dot(r.gs[mine, :], r.wo[:, cols(opp)]).astype(BF16)
                far_p(ready).start()
                far_m(ready).start()

            @pl.when(k < hc)
            def _():
                gate(seg * hc + k, 0)

            return seg

        def order_of(i):
            past = (i + chunks - first_near) // chunks
            end = (i + 1) // chunks
            return i + (1 - late) * (past - end * (chunks - first_near))

        def near(i, _):
            k = order_of(i)
            mine = crows(k)
            r.txp[mine, :] = dot(r.gs[mine, :], r.wo[:, cols(right)]).astype(BF16)
            r.txm[mine, :] = dot(r.gs[mine, :], r.wo[:, cols(left)]).astype(BF16)
            top = khalf(k, 0)
            got(r.rl.at[kept_half(k), :], r.far_pr.at[k])
            r.txp[top, :] = (
                r.txp[top, :].astype(F32) + r.rl[kept_half(k), :].astype(F32)
            ).astype(BF16)
            near_p(k).start()
            low = khalf(k, 1)
            got(r.rr.at[kept_half(k), :], r.far_mr.at[k])
            r.txm[low, :] = (
                r.txm[low, :].astype(F32) + r.rr[kept_half(k), :].astype(F32)
            ).astype(BF16)
            near_m(k).start()
            return 0

        def segment(seg, _):
            take_prefixes(seg)
            lax.fori_loop(0, hc + lag, far, seg)

            @pl.when(seg == 0)
            def _():
                send_prefixes(1)
                lax.fori_loop(half_blocks, blocks, lambda b, _: (project_gate(b), 0)[1], 0)
                lax.fori_loop(0, held, near, 0)

            return 0

        lax.fori_loop(0, 2, segment, 0)
        r.pkt[...] = r.peak[...]

        def peak_to(off):
            q = lax.rem(at + off, n_seq)
            return to_seq(r.pkt, r.pkr.at[at], r.pk_s.at[0], r.pk_r.at[0], q)

        def peak_send(off, _):
            peak_to(off).start()
            return 0

        lax.fori_loop(1, n_seq, peak_send, 0)
        r.pkr[at] = r.peak[...]

        lax.fori_loop(first_near, chunks, near, 0)

        def back(j):
            here = pl.ds(pl.multiple_of(j * CHUNK, CHUNK), CHUNK)
            return to_seq(r.otx.at[here, :], r.orx.at[here, :],
                          r.out_s.at[0], r.out_r.at[j], mate)

        def finish(i, _):
            k = order_of(i)
            mine = crows(k)
            total = dot(r.gs[mine, :], r.wo[:, cols(me)])
            got(r.rxp.at[mine, :], r.near_pr.at[k])
            got(r.rxm.at[mine, :], r.near_mr.at[k])
            total = total + (r.rxp[mine, :].astype(F32) + r.rxm[mine, :].astype(F32))
            out = (total * unscale[0:1, 0:1]).astype(BF16)
            j = lax.rem(k, hc)
            here = pl.ds(pl.multiple_of(j * CHUNK, CHUNK), CHUNK)

            @pl.when(k // hc == late)
            def _():
                r.mixed[here, :] = out

            @pl.when(k // hc != late)
            def _():
                r.otx[here, :] = out
                back(j).start()

            return 0

        lax.fori_loop(0, chunks, finish, 0)
        for j in range(hc):
            got(r.orx.at[pl.ds(j * CHUNK, CHUNK), :], r.out_r.at[j])
            to = half_rows + j * CHUNK
            r.mixed[to : to + CHUNK, :] = r.orx[j * CHUNK : (j + 1) * CHUNK, :]
        got(r.pkr.at[others], r.pk_r.at[0])
        top = lax.fori_loop(0, n_seq, lambda j, v: jnp.maximum(v, r.pkr[j]), r.peak[...])
        lane = lax.broadcasted_iota(jnp.int32, r.news.shape, 1)
        news = jnp.broadcast_to(jnp.max(top, axis=1, keepdims=True), r.news.shape)
        for i in range(1, r.hist.shape[0]):
            news = jnp.where(lane == i, r.hist[i - 1], news)
        r.news[...] = news

        got(r.tail.at[:, known], r.tail_s.at[0])

        @pl.when(at < n_seq - 1)
        def _():
            rims[0].wait_send()

        rims[1].wait_send()
        half_own = r.h.at[pl.ds(0, rows // 2), own]
        for view, sem in (
            (r.h.at[:, own], r.own_ps), (r.h.at[:, own], r.own_ms),
            (half_own, r.rel_ps), (half_own, r.rel_ms),
            (r.rl, r.far_ps), (r.rr, r.far_ms), (r.txp, r.near_ps), (r.txm, r.near_ms),
            (r.swap, r.swap_s), (r.otx, r.out_s), (r.pkr.at[others], r.pk_s),
            (r.stat.at[pl.ds(0, n_tp - 1)], r.sa_s),
        ):
            got(view, sem.at[0])
        for seg in range(2):
            got(r.drx.at[seg, others], r.dc_s.at[seg])
            got(r.srx.at[seg, others], r.st_s.at[seg])
            got(r.prx.at[seg, others], r.pf_s.at[seg])

    hbm = pl.BlockSpec(memory_space=pl.ANY)
    local = pl.BlockSpec(memory_space=pltpu.VMEM)
    scalars = pl.BlockSpec(memory_space=pltpu.SMEM)
    return pl.pallas_call(
        kernel,
        name="layer",
        out_shape=(
            pltpu.VMEM((rows, part), BF16),
            pltpu.VMEM((1, 16), F32),
        ),
        in_specs=[hbm] * 14 + [scalars],
        out_specs=(local, local),
        scratch_shapes=[pltpu.VMEM(*v) for v in (*vmem.values(), *small.values())]
        + [pltpu.SemaphoreType.DMA((n,)) for n in dma.values()],
        compiler_params=pltpu.CompilerParams(
            collective_id=0, has_side_effects=True, vmem_limit_bytes=65_650_000
        ),
    )


def solution(mesh):
    n_seq, n_tp = mesh.shape["seq"], mesh.shape["tp"]
    side = max(k for k in range(1, n_seq) if 2 * k * k <= n_seq and n_seq % (2 * k) == 0)
    split = (n_seq // (2 * side), side, 2)

    def shards(
        hidden, gate_proj, input_proj, bc_proj, step_proj, step_bias, decay_log, conv_weight,
        conv_bias, bc_conv_weight, bc_conv_bias, skip_gain, norm_gain, out_proj, amax_history,
    ):
        rows, part = hidden.shape
        call = build(rows, part, gate_proj.shape[1], n_tp, n_seq, step_proj.shape[1], split)
        mixed, news = call(
            hidden, gate_proj, input_proj, bc_proj, step_proj.T, step_bias[None], decay_log[None],
            conv_weight, conv_bias.reshape(-1, LANES), bc_conv_weight, bc_conv_bias[None],
            skip_gain[None], norm_gain.reshape(-1, LANES), out_proj, amax_history,
        )
        return mixed, news.reshape(-1)

    cols = P(None, "tp")
    flat = P("tp")
    in_specs = (
        P("seq", "tp"), cols, cols, P(), cols, flat, flat, cols, flat, P(), P(), flat, flat,
        P("tp", None), P(),
    )
    return jax.shard_map(
        shards, mesh=mesh, in_specs=in_specs, out_specs=(P("seq", "tp"), P()), check_vma=False
    )
```
